256 devices in a mesh: row: 16 (over z_hi, y, core), col: 16 (over x, z_lo).
Axes of the slice: x: 4, y: 4, z: 8 (z_hi: 2, z_lo: 4; z = z_hi * 4 + z_lo), core: 2. Of those that a mesh axis runs over, the one named last changes fastest.
Arguments:
- constraint_blocks: float32 [64, 32, 256, 256], P('row', 'col'), may hold values from -0.0625 to 0.0625
- factor_blocks: float32 [64, 32, 256, 256], P('row', 'col'), may hold values from -0.0625 to 0.0625
- band_offsets: int32 [16, 2], P('col'), may hold values from 0 to 63, as said below
- block_pattern: int32 [64, 32], P('row', 'col'), may hold values 0 or 1
- cost_linear: float32 [262144], P('col'), may hold values from -6 to 6
- cost_diagonal: float32 [262144], P('col'), may hold values from 0.5 to 4
- lower: float32 [16384], P('row'), may hold values from -1.5 to -0.2
- upper: float32 [16384], P('row'), may hold values from 0.2 to 1.5
- x_start: float32 [262144], P('col'), may hold values from -6 to 6
- z_start: float32 [16384], P('row'), may hold values from -1 to 1
- y_start: float32 [16384], P('row'), may hold values from -0.6 to 0.6
Outputs:
- x_final: float32 [262144], P('col')
- z_final: float32 [16384], P('row')
- y_final: float32 [16384], P('row')
- residuals: float32 [2, 2], replicated
The draws below stay inside these ranges and needn't reach their ends.
Inputs may be any that keep to these rules, and one draw needn't show every extreme that they name: In each row of band_offsets the 2 offsets are distinct.
All inputs are finite; a program needn't handle non-finite values. No bound on the sum of `block_pattern` on one device may be relied on, other than what follows from the above.
Results may differ from the reference program's by a relative error of at most 0.00016.
Values sent between devices are 32-bit elements; how exact they have to be, the bound alone decides.
No kernel may reach another device: no remote copies, remote signals or barrier semaphores. Data moves between devices by JAX's collectives and lax.ppermute only.
A program may use at most 64 MiB of HBM per device.

```python
import math
import jax
import jax.numpy as jnp
from jax import lax

BS = 256
KB = 2
CBD = 64
ITERS = 2
CG_STEPS = 2
GROUPS = 16
BANDS = 32
NBR = 64
NBC = 1024
MROWS = 16384
NVARS = 262144


def draw_band_offsets(key, part):
    keys = jax.random.split(jax.random.fold_in(key, 17), GROUPS)

    def one_group(group_key):
        return jax.random.permutation(group_key, CBD)[:KB].astype(jnp.int32)
    return jax.vmap(one_group)(keys).astype(jnp.int32)


def set_ends(array, stream_key, low, largest):
    dims = array.shape
    place = [jax.random.randint(jax.random.fold_in(stream_key, axis), (), 0, dims[axis]) for axis in range(len(dims))]
    array = array.at[tuple(place)].set(low)
    longest = dims.index(max(dims))
    place[longest] = (place[longest] + 1) % dims[longest]
    return array.at[tuple(place)].set(largest)


def levels(own_key, dims, cuts, smallest, top_value):
    def one(axis_at, parts):
        heights = jax.random.uniform(jax.random.fold_in(jax.random.fold_in(own_key, 6), axis_at), (parts,), jnp.float32, smallest / len(cuts), top_value / len(cuts))
        return jnp.repeat(jnp.exp(heights), dims[axis_at] // parts).reshape((-1,) + (1,) * (len(dims) - axis_at - 1))

    level = one(*cuts[0])
    for cut in cuts[1:]:
        level = level * one(*cut)
    return level


def normal_values(stream_key, dims, spread, bound, cuts=(), kind=jnp.bfloat16):
    factor_of = levels(stream_key, dims, cuts, -0.22, 0.18) if cuts else 1.0
    array = jax.random.normal(stream_key, dims, jnp.float32) * spread * factor_of
    return jnp.minimum(jnp.maximum(array, -bound), bound).astype(kind)


def setup_inputs(seed: int = 0) -> dict:
    splits = jax.random.split(jax.random.key(seed), 12)
    constraint_blocks = normal_values(splits[0], (NBR, BANDS, BS, BS), (BANDS * BS) ** -0.5, 0.0625, ((0, 16), (1, 16)), jnp.float32)
    factor_blocks = normal_values(splits[1], (NBR, BANDS, BS, BS), (BANDS * BS) ** -0.5, 0.0625, ((0, 16), (1, 16)), jnp.float32)
    band_offsets = draw_band_offsets(jax.random.fold_in(splits[11], 71), 0)
    block_pattern = set_ends((jax.random.randint(splits[3], (NBR, BANDS), 0, 4) < 3).astype(jnp.int32), jax.random.fold_in(splits[3], 1), 0, 1)
    cost_linear = normal_values(splits[4], (NVARS,), 1.0, 6.0, ((0, 16),), jnp.float32)
    cost_diagonal = jnp.clip(jnp.exp(math.log(4.0) - 2.0794415 * jax.random.uniform(splits[5], (NVARS,), jnp.float32) ** levels(splits[5], (NVARS,), ((0, 16),), -0.2, 0.2)), 0.5, 4.0)
    lower = jnp.clip(-1.5 + 1.3 * jax.random.uniform(splits[6], (MROWS,), jnp.float32) ** levels(splits[6], (MROWS,), ((0, 16),), -0.2, 0.2), -1.5, -0.2)
    upper = jnp.clip(0.2 + 1.3 * jax.random.uniform(splits[7], (MROWS,), jnp.float32) ** levels(splits[7], (MROWS,), ((0, 16),), -0.2, 0.2), 0.2, 1.5)
    x_start = normal_values(splits[8], (NVARS,), 1.0, 6.0, ((0, 16),), jnp.float32)
    z_start = jnp.clip(jax.random.uniform(splits[9], (MROWS,), jnp.float32, -1.0, 1.0) * levels(splits[9], (MROWS,), ((0, 16),), -0.4, 0.0), -1.0, 1.0)
    y_start = normal_values(splits[10], (MROWS,), 0.1, 0.6, ((0, 16),), jnp.float32)
    return {"constraint_blocks": constraint_blocks, "factor_blocks": factor_blocks, "band_offsets": band_offsets, "block_pattern": block_pattern, "cost_linear": cost_linear, "cost_diagonal": cost_diagonal, "lower": lower, "upper": upper, "x_start": x_start, "z_start": z_start, "y_start": y_start}


sigma_shift = 1e-6
rho_step = 0.1
relaxation = 1.6


def column_map(band_offsets):
    block_rows = jnp.arange(NBR, dtype=jnp.int32)
    group_ids = jnp.arange(GROUPS, dtype=jnp.int32)
    inner = (block_rows[:, None, None] % CBD + band_offsets[None, :, :]) % CBD
    columns = group_ids[None, :, None] * CBD + inner
    return columns.reshape(NBR, BANDS).astype(jnp.int32)


def forward(blocks, pattern, columns, vector):
    vector_blocks = vector.reshape(NBC, BS)
    gathered = vector_blocks[columns] * pattern[:, :, None]
    result = jnp.einsum("ijab,ijb->ia", blocks, gathered, precision=lax.Precision.HIGHEST)
    return result.reshape(-1)


def backward(blocks, pattern, columns, vector):
    vector_blocks = vector.reshape(NBR, BS)
    contrib = jnp.einsum("ijab,ia->ijb", blocks, vector_blocks, precision=lax.Precision.HIGHEST)
    contrib = contrib * pattern[:, :, None]
    summed = jax.ops.segment_sum(contrib.reshape(-1, BS), columns.reshape(-1), num_segments=NBC)
    return summed.reshape(-1)


def reference(constraint_blocks, factor_blocks, band_offsets, block_pattern, cost_linear, cost_diagonal, lower, upper, x_start, z_start, y_start):
    columns = column_map(band_offsets)
    pattern = block_pattern.astype(jnp.float32)
    shifted = cost_diagonal + sigma_shift

    def apply_a(vector):
        return forward(constraint_blocks, pattern, columns, vector)

    def apply_at(vector):
        return backward(constraint_blocks, pattern, columns, vector)

    def apply_gtg(vector):
        return backward(factor_blocks, pattern, columns, forward(factor_blocks, pattern, columns, vector))

    def apply_m(vector):
        return shifted * vector + apply_gtg(vector) + rho_step * apply_at(apply_a(vector))

    iterate, z_value, y_value = x_start, z_start, y_start
    primal_list = []
    dual_list = []
    for outer in range(ITERS):
        rhs = sigma_shift * iterate - cost_linear + apply_at(rho_step * z_value - y_value)
        solved = iterate
        remainder = rhs - apply_m(iterate)
        direction = remainder
        norm_now = jnp.sum(remainder * remainder)
        for inner in range(CG_STEPS):
            image = apply_m(direction)
            step_size = norm_now / jnp.sum(direction * image)
            solved = solved + step_size * direction
            remainder = remainder - step_size * image
            norm_next = jnp.sum(remainder * remainder)
            direction = remainder + (norm_next / norm_now) * direction
            norm_now = norm_next
        z_tilde = apply_a(solved)
        iterate = relaxation * solved + (1.0 - relaxation) * iterate
        blended = relaxation * z_tilde + (1.0 - relaxation) * z_value
        z_new = jnp.minimum(jnp.maximum(blended + y_value / rho_step, lower), upper)
        y_value = y_value + rho_step * (blended - z_new)
        z_value = z_new
        primal_list.append(jnp.max(jnp.abs(apply_a(iterate) - z_value)))
        dual_vec = cost_diagonal * iterate + apply_gtg(iterate) + cost_linear + apply_at(y_value)
        dual_list.append(jnp.max(jnp.abs(dual_vec)))
    residuals = jnp.stack([jnp.stack(primal_list), jnp.stack(dual_list)])
    return iterate, z_value, y_value, residuals
```

```python
import jax
import jax.numpy as jnp
from jax import lax
from jax.experimental import pallas as pl
from jax.experimental.pallas import tpu as pltpu
from jax.sharding import Mesh
from jax.sharding import PartitionSpec as P

BS = 256
LANES = 128
ROW = ("row_0", "row_1", "row_2")
COL = ("col_0", "col_1")
PEERS = 16
VROWS = 128

sigma_shift = 1e-06
rho_step = 0.1
relaxation = 1.6

f32 = jnp.float32
VMEM = pl.BlockSpec(memory_space=pltpu.VMEM)
SMEM = pl.BlockSpec(memory_space=pltpu.SMEM)


def kernel_call(body, name, outs, scratch=()):
    def call(meta, *arrays):
        return pl.pallas_call(
            body,
            name=name,
            out_shape=[jax.ShapeDtypeStruct(s, f32) for s in outs],
            in_specs=[SMEM] + [VMEM] * len(arrays),
            out_specs=[VMEM] * len(outs),
            scratch_shapes=[pltpu.VMEM(s, f32) for s in scratch],
            compiler_params=pltpu.CompilerParams(vmem_limit_bytes=4 << 20),
        )(meta, *arrays)

    return call


def row_sum(a):
    return jnp.sum(a, axis=0, keepdims=True)


def forward(mat, touched, out, at):
    for t in range(4):
        for ha in range(2):
            acc = None
            for k in range(2):
                for lt in range(2):
                    j = 2 * t + lt
                    tile = mat[t, k, ha * LANES : (ha + 1) * LANES, lt * LANES : (lt + 1) * LANES]
                    term = tile * touched[k][j : j + 1, :]
                    acc = term if acc is None else acc + term
            j = at + 2 * t + ha
            out[j : j + 1, :] = row_sum(acc.T)


def backward(pairs, pattern, out, at):
    for t in range(4):
        acc = [[None, None], [None, None]]
        for mat, v in pairs:
            for ha in range(2):
                j = 2 * t + ha
                column = jnp.broadcast_to(v[j : j + 1, :], (LANES, LANES)).T
                for k in range(2):
                    for lt in range(2):
                        tile = mat[t, k, ha * LANES : (ha + 1) * LANES, lt * LANES : (lt + 1) * LANES]
                        part = (tile * column).reshape(16, 8, LANES).sum(axis=0)
                        acc[k][lt] = part if acc[k][lt] is None else acc[k][lt] + part
        for k in range(2):
            for lt in range(2):
                j = 2 * t + lt
                out[at + 8 * k + j : at + 8 * k + j + 1, :] = (
                    row_sum(acc[k][lt]) * pattern[k, j : j + 1, :]
                )


def gather_touched(meta, vector, pattern, ring):
    ring[0:VROWS, :] = vector
    ring[VROWS : VROWS + 8, :] = vector[0:8, :]
    return [ring[pl.ds(meta[2 + k], 8), :] * pattern[k] for k in range(2)]


def assemble(meta, received, at, turn):
    total = None
    for k in range(2):
        for peer in range(PEERS):
            part = received[peer, at + 8 * k : at + 8 * k + 8, :]
            turn[k, 8 * peer : 8 * peer + 8, :] = part
            turn[k, VROWS + 8 * peer : VROWS + 8 * peer + 8, :] = part
        turned = turn[k, pl.ds(meta[k], VROWS), :]
        total = turned if total is None else total + turned
    return total


def to_all(line, out):
    value = line[...]
    for peer in range(PEERS):
        out[peer, :, :] = value


def peer_total(received, lo, hi):
    total = received[0, lo:hi, :]
    for peer in range(1, PEERS):
        total = total + received[peer, lo:hi, :]
    return total


def peer_max(received, lo, hi):
    total = received[0, lo:hi, :]
    for peer in range(1, PEERS):
        total = jnp.maximum(total, received[peer, lo:hi, :])
    return total


def lane_total(a):
    return jnp.sum(a, axis=1, keepdims=True)


def products_of(meta, vector, mats, pattern, ring, line):
    touched = gather_touched(meta, vector, pattern, ring)
    forward(mats[0], touched, line, 0)
    forward(mats[1], touched, line, 8)


def first_products(meta, A, G, pat, x, out, line, ring):
    products_of(meta, x[...], (G, A), pat, ring, line)
    to_all(line, out)


def start_rows(z, y, gx, ax):
    return rho_step * z - y - rho_step * ax, -gx


def first_start(meta, A, G, pat, recv, z, y, out, gx_out, ax_out, line):
    gx = peer_total(recv, 0, 8)
    ax = peer_total(recv, 8, 16)
    gx_out[...] = gx
    ax_out[...] = ax
    va, vg = start_rows(z[...], y[...], gx, ax)
    backward(((A, va), (G, vg)), pat, line, 0)
    to_all(line, out)


def begin_solve(meta, A, G, pat, recv, x, diag, lin, out, rem_out, *rest, dual):
    if dual:
        dual_out, line, ring, turn = rest
    else:
        line, ring, turn = rest
    start = assemble(meta, recv, 0, turn)
    xv = x[...]
    shifted = diag[...] + sigma_shift
    rem = sigma_shift * xv - lin[...] - shifted * xv + start
    rem_out[...] = rem
    products_of(meta, rem, (G, A), pat, ring, line)
    line[16:17, :] = row_sum(rem * rem)
    line[17:18, :] = row_sum(rem * shifted * rem)
    line[18:24, :] = jnp.zeros((6, LANES), f32)
    to_all(line, out)
    if dual:
        residual = diag[...] * xv + lin[...] + assemble(meta, recv, 16, turn)
        dual_out[...] = jnp.max(jnp.abs(residual), axis=0, keepdims=True)


def first_image(meta, A, G, pat, recv, out, gd_out, ad_out, sc_out, line):
    gd = peer_total(recv, 0, 8)
    ad = peer_total(recv, 8, 16)
    gd_out[...] = gd
    ad_out[...] = ad
    sc_out[...] = peer_total(recv, 16, 24)
    backward(((G, gd), (A, rho_step * ad)), pat, line, 0)
    line[16:17, :] = row_sum(gd * gd + rho_step * (ad * ad))
    line[17:24, :] = jnp.zeros((7, LANES), f32)
    to_all(line, out)


def first_step(meta, A, G, pat, recv, direction, sc, diag, out, rem_out, step_out, line, ring, turn):
    image_part = assemble(meta, recv, 0, turn)
    squares = lane_total(peer_total(recv, 16, 24))[0:1, :]
    scalars = lane_total(sc[...])
    norm, weighted = scalars[0:1, :], scalars[1:2, :]
    step = norm / (squares + weighted)
    d = direction[...]
    shifted = diag[...] + sigma_shift
    rem = d - step * (image_part + shifted * d)
    rem_out[...] = rem
    step_out[...] = jnp.broadcast_to(step, (8, LANES))
    products_of(meta, rem, (G, A), pat, ring, line)
    weighted_rem = rem * shifted
    line[16:17, :] = row_sum(rem * rem)
    line[17:18, :] = row_sum(weighted_rem * rem)
    line[18:19, :] = row_sum(weighted_rem * d)
    line[19:24, :] = jnp.zeros((5, LANES), f32)
    to_all(line, out)


def second_images(meta, recv, gd, ad, sc, out, gd_out, ad_out, small_out):
    scalars = lane_total(peer_total(recv, 16, 24))
    norm, weighted_rem, weighted_mix = scalars[0:1, :], scalars[1:2, :], scalars[2:3, :]
    before = lane_total(sc[...])
    norm_old, weighted_old = before[0:1, :], before[1:2, :]
    ratio = norm / norm_old
    gd2 = peer_total(recv, 0, 8) + ratio * gd[...]
    ad2 = peer_total(recv, 8, 16) + ratio * ad[...]
    gd_out[...] = gd2
    ad_out[...] = ad2
    weighted = weighted_rem + 2.0 * ratio * weighted_mix + ratio * ratio * weighted_old
    small_out[0:1, :] = jnp.broadcast_to(norm, (1, LANES))
    small_out[1:2, :] = jnp.broadcast_to(weighted, (1, LANES))
    small_out[2:3, :] = jnp.broadcast_to(ratio, (1, LANES))
    small_out[3:8, :] = jnp.zeros((5, LANES), f32)
    squares = gd2 * gd2 + rho_step * (ad2 * ad2)
    for peer in range(PEERS):
        out[peer, :, :] = squares


def update(
    meta, A, G, pat, recv, small, step, gd, ad, gd2, ad2, gx, ax, x, rem, d, z, y, lo, hi,
    *rest, last,
):
    if last:
        primal0, out, x_out, z_out, y_out, line = rest
    else:
        out, x_out, z_out, y_out, gx_out, ax_out, primal_out, line = rest
    squares = lane_total(row_sum(peer_total(recv, 0, 8)))
    sm = small[...]
    norm, weighted, ratio = sm[0:1, :], sm[1:2, :], sm[2:3, :]
    step2 = norm / (squares + weighted)
    step1 = step[0:1, :]
    dv = d[...]
    xv = x[...]
    solved = xv + step1 * dv + step2 * (rem[...] + ratio * dv)
    x_out[...] = relaxation * solved + (1.0 - relaxation) * xv
    axv = ax[...]
    tracked = axv + step1 * ad[...] + step2 * ad2[...]
    zv, yv = z[...], y[...]
    blended = relaxation * tracked + (1.0 - relaxation) * zv
    z_new = jnp.minimum(jnp.maximum(blended + yv / rho_step, lo[...]), hi[...])
    y_new = yv + rho_step * (blended - z_new)
    z_out[...] = z_new
    y_out[...] = y_new
    gxv = gx[...]
    gx_new = relaxation * (gxv + step1 * gd[...] + step2 * gd2[...]) + (1.0 - relaxation) * gxv
    ax_new = relaxation * tracked + (1.0 - relaxation) * axv
    primal = jnp.max(jnp.abs(ax_new - z_new), axis=0, keepdims=True)
    if last:
        backward(((G, gx_new), (A, y_new)), pat, line, 0)
        line[16:17, :] = primal0[...]
        line[17:18, :] = primal
        line[18:24, :] = jnp.zeros((6, LANES), f32)
    else:
        gx_out[...] = gx_new
        ax_out[...] = ax_new
        primal_out[...] = primal
        va, vg = start_rows(z_new, y_new, gx_new, ax_new)
        backward(((A, va), (G, vg)), pat, line, 0)
        backward(((G, gx_new), (A, y_new)), pat, line, 16)
    to_all(line, out)


def last_dual(meta, recv, x, diag, lin, dual0, out, turn):
    residual = diag[...] * x[...] + lin[...] + assemble(meta, recv, 0, turn)
    primal = peer_max(recv, 16, 24)
    dual = jnp.max(jnp.abs(residual), axis=0, keepdims=True)
    value = jnp.concatenate([primal[0:2, :], dual0[...], dual, jnp.zeros((4, LANES), f32)], axis=0)
    for peer in range(PEERS):
        out[peer, :, :] = value


def finish(meta, recv, out):
    top = jnp.max(peer_max(recv, 0, 8), axis=1, keepdims=True)
    out[0:1, 0:1] = top[0:1, :]
    out[0:1, 1:2] = top[1:2, :]
    out[1:2, 0:1] = top[2:3, :]
    out[1:2, 1:2] = top[3:4, :]


V = (VROWS, LANES)
R8 = (8, LANES)
ONE = (1, LANES)
RING = (VROWS + 8, LANES)
TURN = (2, 2 * VROWS, LANES)


def payload(rows):
    return (PEERS, rows, LANES)


def exchange(a, axes):
    return lax.all_to_all(a, axes, 0, 0, tiled=True)


def local(
    constraint_blocks, factor_blocks, band_offsets, block_pattern, cost_linear, cost_diagonal,
    lower, upper, x_start, z_start, y_start,
):
    A, G = constraint_blocks, factor_blocks
    offsets = band_offsets[0]
    first_row = lax.axis_index(ROW) * 4
    meta = jnp.concatenate([VROWS - 2 * offsets, 2 * ((first_row + offsets) % 64)])
    pat = jnp.broadcast_to(
        block_pattern.astype(f32).T[:, :, None, None], (2, 4, 2, LANES)
    ).reshape(2, 8, LANES)
    lin, diag = cost_linear.reshape(V), cost_diagonal.reshape(V)
    lo, hi = lower.reshape(R8), upper.reshape(R8)
    x, z, y = x_start.reshape(V), z_start.reshape(R8), y_start.reshape(R8)

    (out,) = kernel_call(first_products, "first_products", [payload(16)], [(16, LANES), RING])(
        meta, A, G, pat, x
    )
    recv = exchange(out, COL)
    out, gx, ax = kernel_call(first_start, "first_start", [payload(16), R8, R8], [(16, LANES)])(
        meta, A, G, pat, recv, z, y
    )
    primal0 = dual0 = None
    for outer in range(2):
        recv = exchange(out, ROW)
        shapes = [payload(24), V] + ([ONE] if outer else [])

        def body(*refs, dual=bool(outer)):
            begin_solve(*refs, dual=dual)

        got = kernel_call(body, f"begin_solve_{outer}", shapes, [(24, LANES), RING, TURN])(
            meta, A, G, pat, recv, x, diag, lin
        )
        out, d = got[:2]
        if outer:
            dual0 = got[2]
        recv = exchange(out, COL)
        out, gd, ad, sc = kernel_call(
            first_image, "first_image", [payload(24), R8, R8, R8], [(24, LANES)]
        )(meta, A, G, pat, recv)
        recv = exchange(out, ROW)
        out, rem, step = kernel_call(
            first_step, "first_step", [payload(24), V, R8], [(24, LANES), RING, TURN]
        )(meta, A, G, pat, recv, d, sc, diag)
        recv = exchange(out, COL)
        out, gd2, ad2, small = kernel_call(second_images, "second_images", [payload(8), R8, R8, R8])(
            meta, recv, gd, ad, sc
        )
        recv = exchange(out, ROW)
        args = (meta, A, G, pat, recv, small, step, gd, ad, gd2, ad2, gx, ax, x, rem, d, z, y, lo, hi)
        if outer == 0:

            def body(*refs):
                update(*refs, last=False)

            out, x, z, y, gx, ax, primal0 = kernel_call(
                body, "update_0", [payload(32), V, R8, R8, R8, R8, ONE], [(32, LANES)]
            )(*args)
        else:

            def body(*refs):
                update(*refs, last=True)

            out, x, z, y = kernel_call(body, "update_1", [payload(24), V, R8, R8], [(24, LANES)])(
                *args, primal0
            )
    recv = exchange(out, ROW)
    (out,) = kernel_call(last_dual, "last_dual", [payload(8)], [TURN])(meta, recv, x, diag, lin, dual0)
    recv = exchange(out, COL)
    (residuals,) = kernel_call(finish, "finish", [(2, 2)])(meta, recv)
    return x.reshape(-1), z.reshape(-1), y.reshape(-1), residuals


def solution(mesh):
    torus = Mesh(mesh.devices.reshape(2, 4, 2, 4, 4), ROW + COL)
    in_specs = (
        P(ROW, COL, None, None), P(ROW, COL, None, None), P(COL, None), P(ROW, COL), P(COL), P(COL),
        P(ROW), P(ROW), P(COL), P(ROW), P(ROW),
    )
    out_specs = (P(COL), P(ROW), P(ROW), P())
    return jax.shard_map(local, mesh=torus, in_specs=in_specs, out_specs=out_specs, check_vma=False)
```

```python
import jax
import jax.numpy as jnp
from jax import lax
from jax.experimental import pallas as pl
from jax.experimental.pallas import tpu as pltpu
from jax.sharding import Mesh
from jax.sharding import PartitionSpec as P

BS = 256
LANES = 128
ROW = ("row_0", "row_1", "row_2")
COL = ("col_0", "col_1")
PEERS = 16
VROWS = 128

sigma_shift = 1e-06
rho_step = 0.1
relaxation = 1.6

f32 = jnp.float32
VMEM = pl.BlockSpec(memory_space=pltpu.VMEM)
SMEM = pl.BlockSpec(memory_space=pltpu.SMEM)


def kernel_call(body, name, outs, scratch=(), spaces=None):
    def call(*arrays):
        return pl.pallas_call(
            body,
            name=name,
            out_shape=[jax.ShapeDtypeStruct(s, f32) for s in outs],
            in_specs=spaces or [SMEM] + [VMEM] * (len(arrays) - 1),
            out_specs=[VMEM] * len(outs),
            scratch_shapes=[pltpu.VMEM(s, f32) if isinstance(s, tuple) else s for s in scratch],
            compiler_params=pltpu.CompilerParams(vmem_limit_bytes=8 << 20),
        )(*arrays)

    return call


def row_sum(a):
    return jnp.sum(a, axis=0, keepdims=True)


def forward_row(mat, t, touched, out, at):
    for ha in range(2):
        acc = None
        for k in range(2):
            for lt in range(2):
                j = 2 * t + lt
                tile = mat[t, k, ha * LANES : (ha + 1) * LANES, lt * LANES : (lt + 1) * LANES]
                term = tile * touched[k][j : j + 1, :]
                acc = term if acc is None else acc + term
        j = at + 2 * t + ha
        out[j : j + 1, :] = row_sum(acc.T)


def forward(mat, touched, out, at):
    for t in range(4):
        forward_row(mat, t, touched, out, at)


def backward(pairs, pattern, out, at):
    for t in range(4):
        acc = [[None, None], [None, None]]
        for mat, v in pairs:
            for ha in range(2):
                j = 2 * t + ha
                column = jnp.broadcast_to(v[j : j + 1, :], (LANES, LANES)).T
                for k in range(2):
                    for lt in range(2):
                        tile = mat[t, k, ha * LANES : (ha + 1) * LANES, lt * LANES : (lt + 1) * LANES]
                        part = (tile * column).reshape(16, 8, LANES).sum(axis=0)
                        acc[k][lt] = part if acc[k][lt] is None else acc[k][lt] + part
        for k in range(2):
            for lt in range(2):
                j = 2 * t + lt
                out[at + 8 * k + j : at + 8 * k + j + 1, :] = (
                    row_sum(acc[k][lt]) * pattern[k, j : j + 1, :]
                )


def first_touched(offsets, k):
    return 2 * ((lax.axis_index(ROW) * 4 + offsets[0, k]) % 64)


def gather_touched(offsets, vector, pattern, ring):
    ring[0:VROWS, :] = vector
    ring[VROWS : VROWS + 8, :] = vector[0:8, :]
    return [ring[pl.ds(first_touched(offsets, k), 8), :] * pattern[k] for k in range(2)]


def assemble(offsets, received, each, at, turn):
    total = None
    for k in range(2):
        for peer in range(PEERS):
            lo = each * peer + at + 8 * k
            part = received[lo : lo + 8, :]
            turn[k, 8 * peer : 8 * peer + 8, :] = part
            turn[k, VROWS + 8 * peer : VROWS + 8 * peer + 8, :] = part
        turned = turn[k, pl.ds(VROWS - 2 * offsets[0, k], VROWS), :]
        total = turned if total is None else total + turned
    return total


def to_all(line, out):
    each = out.shape[0] // PEERS
    value = line[0:each, :]
    for peer in range(PEERS):
        out[each * peer : each * (peer + 1), :] = value


def peer_total(received, each, lo, hi):
    total = received[lo:hi, :]
    for peer in range(1, PEERS):
        total = total + received[each * peer + lo : each * peer + hi, :]
    return total


def lane_total(a):
    return jnp.sum(a, axis=1, keepdims=True)


def full_total(a):
    return lane_total(row_sum(a))


def full_max(a):
    return jnp.max(jnp.max(a, axis=0, keepdims=True), axis=1, keepdims=True)


def packed(values):
    lane = lax.broadcasted_iota(jnp.int32, (1, LANES), 1)
    row = jnp.zeros((1, LANES), f32)
    for n, value in enumerate(values):
        row = jnp.where(lane == n, value, row)
    return row


def products_of(offsets, vector, mats, pattern, ring, line):
    touched = gather_touched(offsets, vector, pattern, ring)
    forward(mats[0], touched, line, 0)
    forward(mats[1], touched, line, 8)


def first_products(
    offsets_in, pattern_in, A_in, G_in, x_in, out, pat_out, A, G,
    offsets, pattern, line, ring, small_sems, sems,
):
    small = [
        pltpu.make_async_copy(offsets_in, offsets, small_sems.at[0]),
        pltpu.make_async_copy(pattern_in, pattern, small_sems.at[1]),
        pltpu.make_async_copy(x_in, ring.at[0:VROWS, :], small_sems.at[2]),
        pltpu.make_async_copy(x_in.at[0:8, :], ring.at[VROWS : VROWS + 8, :], small_sems.at[3]),
    ]
    big = [
        [pltpu.make_async_copy(src.at[t], dst.at[t], sems.at[m, t]) for t in range(4)]
        for m, (src, dst) in enumerate(((G_in, G), (A_in, A)))
    ]
    for copy in small + big[0] + big[1]:
        copy.start()
    for copy in small:
        copy.wait()
    for k in range(2):
        for t in range(4):
            pat_out[k, 2 * t : 2 * t + 2, :] = jnp.full((2, LANES), pattern[k, t].astype(f32))
    touched = [ring[pl.ds(first_touched(offsets, k), 8), :] * pat_out[k] for k in range(2)]
    for m, mat in enumerate((G, A)):
        for t in range(4):
            big[m][t].wait()
            forward_row(mat, t, touched, line, 8 * m)
    to_all(line, out)


def start_rows(z, y, gx, ax):
    return rho_step * z - y - rho_step * ax, -gx


def first_start(offsets, A, G, pat, recv, z, y, out, gx_out, ax_out, line):
    gx = peer_total(recv, 16, 0, 8)
    ax = peer_total(recv, 16, 8, 16)
    gx_out[...] = gx
    ax_out[...] = ax
    va, vg = start_rows(z[...], y[...], gx, ax)
    backward(((A, va), (G, vg)), pat, line, 0)
    to_all(line, out)


def begin_solve(offsets, A, G, pat, recv, x, diag, lin, out, rem_out, *rest, dual):
    if dual:
        dual_out, line, ring, turn = rest
    else:
        line, ring, turn = rest
    each = 32 if dual else 16
    start = assemble(offsets, recv, each, 0, turn)
    xv = x[...]
    shifted = diag[...] + sigma_shift
    rem = sigma_shift * xv - lin[...] - shifted * xv + start
    rem_out[...] = rem
    products_of(offsets, rem, (G, A), pat, ring, line)
    line[16:17, :] = packed((full_total(rem * rem), full_total(rem * shifted * rem)))
    to_all(line, out)
    if dual:
        residual = diag[...] * xv + lin[...] + assemble(offsets, recv, each, 16, turn)
        dual_out[...] = jnp.max(jnp.abs(residual), axis=0, keepdims=True)


def first_image(offsets, A, G, pat, recv, out, gd_out, ad_out, sc_out, line):
    gd = peer_total(recv, 17, 0, 8)
    ad = peer_total(recv, 17, 8, 16)
    gd_out[...] = gd
    ad_out[...] = ad
    sc_out[...] = peer_total(recv, 17, 16, 17)
    backward(((G, gd), (A, rho_step * ad)), pat, line, 0)
    line[16:17, :] = row_sum(gd * gd + rho_step * (ad * ad))
    to_all(line, out)


def first_step(
    offsets, A, G, pat, recv, direction, sc, diag, out, rem_out, step_out, line, ring, turn
):
    image_part = assemble(offsets, recv, 17, 0, turn)
    squares = lane_total(peer_total(recv, 17, 16, 17))
    norm, weighted = sc[0:1, 0:1], sc[0:1, 1:2]
    step = norm / (squares + weighted)
    d = direction[...]
    shifted = diag[...] + sigma_shift
    rem = d - step * (image_part + shifted * d)
    rem_out[...] = rem
    step_out[...] = jnp.broadcast_to(step, (1, LANES))
    products_of(offsets, rem, (G, A), pat, ring, line)
    weighted_rem = rem * shifted
    line[16:17, :] = packed(
        (full_total(rem * rem), full_total(weighted_rem * rem), full_total(weighted_rem * d))
    )
    to_all(line, out)


def second_images(offsets, recv, gd, ad, sc, out, gd_out, ad_out, small_out):
    now = peer_total(recv, 17, 16, 17)
    norm, weighted_rem, weighted_mix = now[:, 0:1], now[:, 1:2], now[:, 2:3]
    norm_old, weighted_old = sc[0:1, 0:1], sc[0:1, 1:2]
    ratio = norm / norm_old
    gd2 = peer_total(recv, 17, 0, 8) + ratio * gd[...]
    ad2 = peer_total(recv, 17, 8, 16) + ratio * ad[...]
    gd_out[...] = gd2
    ad_out[...] = ad2
    weighted = weighted_rem + 2.0 * ratio * weighted_mix + ratio * ratio * weighted_old
    small_out[...] = packed((norm, weighted, ratio))
    squares = row_sum(gd2 * gd2 + rho_step * (ad2 * ad2))
    out[...] = jnp.broadcast_to(squares, (PEERS, LANES))


def update(
    offsets, A, G, pat, recv, small, step, gd, ad, gd2, ad2, gx, ax, x, rem, d, z, y, lo, hi,
    *rest, last,
):
    if last:
        diag, lin, primal0, out, x_out, z_out, y_out, base_out, line = rest
    else:
        out, x_out, z_out, y_out, gx_out, ax_out, primal_out, line = rest
    squares = full_total(recv[...])
    norm, weighted, ratio = small[0:1, 0:1], small[0:1, 1:2], small[0:1, 2:3]
    step2 = norm / (squares + weighted)
    step1 = step[0:1, :]
    axv = ax[...]
    tracked = axv + step1 * ad[...] + step2 * ad2[...]
    zv, yv = z[...], y[...]
    blended = relaxation * tracked + (1.0 - relaxation) * zv
    z_new = jnp.minimum(jnp.maximum(blended + yv / rho_step, lo[...]), hi[...])
    y_new = yv + rho_step * (blended - z_new)
    z_out[...] = z_new
    y_out[...] = y_new
    gxv = gx[...]
    gx_new = relaxation * (gxv + step1 * gd[...] + step2 * gd2[...]) + (1.0 - relaxation) * gxv
    ax_new = relaxation * tracked + (1.0 - relaxation) * axv
    primal = full_max(jnp.abs(ax_new - z_new))
    if last:
        backward(((G, gx_new), (A, y_new)), pat, line, 0)
        line[16:17, :] = packed((primal0[0:1, 0:1], primal))
    else:
        gx_out[...] = gx_new
        ax_out[...] = ax_new
        primal_out[...] = jnp.broadcast_to(primal, (1, LANES))
        va, vg = start_rows(z_new, y_new, gx_new, ax_new)
        backward(((A, va), (G, vg)), pat, line, 0)
        backward(((G, gx_new), (A, y_new)), pat, line, 16)
    to_all(line, out)
    dv = d[...]
    xv = x[...]
    solved = xv + step1 * dv + step2 * (rem[...] + ratio * dv)
    x_new = relaxation * solved + (1.0 - relaxation) * xv
    x_out[...] = x_new
    if last:
        base_out[...] = diag[...] * x_new + lin[...]


def last_dual(offsets, recv, base, dual0, out, turn):
    residual = base[...] + assemble(offsets, recv, 17, 0, turn)
    primal = recv[16:17, :]
    for peer in range(1, PEERS):
        primal = jnp.maximum(primal, recv[17 * peer + 16 : 17 * peer + 17, :])
    row = packed(
        (primal[:, 0:1], primal[:, 1:2], full_max(dual0[...]), full_max(jnp.abs(residual)))
    )
    out[...] = jnp.broadcast_to(row, (PEERS, LANES))


def finish(recv, x, z, y, x_out, z_out, y_out, out):
    x_out[...] = x[...]
    z_out[...] = z[...]
    y_out[...] = y[...]
    top = jnp.max(recv[...], axis=0, keepdims=True)
    out[0:1, :] = top[:, 0:2]
    out[1:2, :] = top[:, 2:4]


V = (VROWS, LANES)
R8 = (8, LANES)
ONE = (1, LANES)
RING = (VROWS + 8, LANES)
TURN = (2, 2 * VROWS, LANES)
BLOCKS = (4, 2, BS, BS)


def payload(rows):
    return (PEERS * rows, LANES)


def exchange(a, axes):
    wide = a.reshape(PEERS, 1, -1)
    return lax.all_to_all(wide, axes, 0, 0, tiled=True).reshape(a.shape)


def local(
    constraint_blocks, factor_blocks, band_offsets, block_pattern, cost_linear, cost_diagonal,
    lower, upper, x_start, z_start, y_start,
):
    A, G, offsets = constraint_blocks, factor_blocks, band_offsets
    lin, diag = cost_linear.reshape(V), cost_diagonal.reshape(V)
    lo, hi = lower.reshape(R8), upper.reshape(R8)
    x, z, y = x_start.reshape(V), z_start.reshape(R8), y_start.reshape(R8)

    out, pat, A, G = kernel_call(
        first_products, "first_products", [payload(16), (2, 8, LANES), BLOCKS, BLOCKS],
        [
            pltpu.SMEM((1, 2), jnp.int32), pltpu.SMEM((2, 4), jnp.int32), (16, LANES), RING,
            pltpu.SemaphoreType.DMA((4,)), pltpu.SemaphoreType.DMA((2, 4)),
        ],
        [pl.BlockSpec(memory_space=pltpu.HBM)] * 5,
    )(*[pltpu.with_memory_space_constraint(a, pltpu.HBM) for a in (offsets, block_pattern.T, A, G, x)])
    recv = exchange(out, COL)
    out, gx, ax = kernel_call(first_start, "first_start", [payload(16), R8, R8], [(16, LANES)])(
        offsets, A, G, pat, recv, z, y
    )
    primal0 = dual0 = None
    for outer in range(2):
        recv = exchange(out, ROW)
        shapes = [payload(17), V] + ([ONE] if outer else [])

        def body(*refs, dual=bool(outer)):
            begin_solve(*refs, dual=dual)

        got = kernel_call(body, f"begin_solve_{outer}", shapes, [(24, LANES), RING, TURN])(
            offsets, A, G, pat, recv, x, diag, lin
        )
        out, d = got[:2]
        if outer:
            dual0 = got[2]
        recv = exchange(out, COL)
        out, gd, ad, sc = kernel_call(
            first_image, "first_image", [payload(17), R8, R8, ONE], [(24, LANES)]
        )(offsets, A, G, pat, recv)
        recv = exchange(out, ROW)
        out, rem, step = kernel_call(
            first_step, "first_step", [payload(17), V, ONE], [(24, LANES), RING, TURN]
        )(offsets, A, G, pat, recv, d, sc, diag)
        recv = exchange(out, COL)
        out, gd2, ad2, small = kernel_call(second_images, "second_images", [payload(1), R8, R8, ONE])(
            offsets, recv, gd, ad, sc
        )
        recv = exchange(out, ROW)
        args = (offsets, A, G, pat, recv, small, step, gd, ad, gd2, ad2, gx, ax, x, rem, d, z, y, lo, hi)
        if outer == 0:

            def body(*refs):
                update(*refs, last=False)

            out, x, z, y, gx, ax, primal0 = kernel_call(
                body, "update_0", [payload(32), V, R8, R8, R8, R8, ONE], [(32, LANES)]
            )(*args)
        else:

            def body(*refs):
                update(*refs, last=True)

            out, x, z, y, base = kernel_call(
                body, "update_1", [payload(17), V, R8, R8, V], [(24, LANES)]
            )(*args, diag, lin, primal0)
    recv = exchange(out, ROW)
    (out,) = kernel_call(last_dual, "last_dual", [payload(1)], [TURN])(offsets, recv, base, dual0)
    recv = exchange(out, COL)
    x, z, y, residuals = kernel_call(finish, "finish", [V, R8, R8, (2, 2)], (), [VMEM] * 4)(recv, x, z, y)
    return x.reshape(-1), z.reshape(-1), y.reshape(-1), residuals


def solution(mesh):
    torus = Mesh(mesh.devices.reshape(2, 4, 2, 4, 4), ROW + COL)
    in_specs = (
        P(ROW, COL, None, None), P(ROW, COL, None, None), P(COL, None), P(ROW, COL), P(COL), P(COL),
        P(ROW), P(ROW), P(COL), P(ROW), P(ROW),
    )
    out_specs = (P(COL), P(ROW), P(ROW), P())
    return jax.shard_map(local, mesh=torus, in_specs=in_specs, out_specs=out_specs, check_vma=False)
```

```python
import jax
import jax.numpy as jnp
from jax import lax
from jax.experimental import pallas as pl
from jax.experimental.pallas import tpu as pltpu
from jax.sharding import Mesh
from jax.sharding import PartitionSpec as P

BS = 256
LANES = 128
ROW = ("row_0", "row_1", "row_2")
COL = ("col_0", "col_1")
PEERS = 16
VROWS = 128

sigma_shift = 1e-06
rho_step = 0.1
relaxation = 1.6

f32 = jnp.float32
VMEM = pl.BlockSpec(memory_space=pltpu.VMEM)


def kernel_call(body, name, outs, scratch=(), spaces=None):
    def call(*arrays):
        return pl.pallas_call(
            body,
            name=name,
            out_shape=[jax.ShapeDtypeStruct(s, f32) for s in outs],
            in_specs=spaces or [VMEM] * len(arrays),
            out_specs=[VMEM] * len(outs),
            scratch_shapes=[pltpu.VMEM(s, f32) if isinstance(s, tuple) else s for s in scratch],
            compiler_params=pltpu.CompilerParams(vmem_limit_bytes=8 << 20),
        )(*arrays)

    return call


def row_sum(a):
    return jnp.sum(a, axis=0, keepdims=True)


def forward_row(mat, t, touched, out, at):
    for ha in range(2):
        acc = None
        for k in range(2):
            for lt in range(2):
                j = 2 * t + lt
                tile = mat[t, k, ha * LANES : (ha + 1) * LANES, lt * LANES : (lt + 1) * LANES]
                term = tile * touched[k][j : j + 1, :]
                acc = term if acc is None else acc + term
        j = at + 2 * t + ha
        out[j : j + 1, :] = row_sum(acc.T)


def forward(mat, touched, out, at):
    for t in range(4):
        forward_row(mat, t, touched, out, at)


def backward(pairs, pattern, out, at):
    for t in range(4):
        acc = [[None, None], [None, None]]
        for mat, v in pairs:
            for ha in range(2):
                j = 2 * t + ha
                column = jnp.broadcast_to(v[j : j + 1, :], (LANES, LANES)).T
                for k in range(2):
                    for lt in range(2):
                        tile = mat[t, k, ha * LANES : (ha + 1) * LANES, lt * LANES : (lt + 1) * LANES]
                        part = (tile * column).reshape(16, 8, LANES).sum(axis=0)
                        acc[k][lt] = part if acc[k][lt] is None else acc[k][lt] + part
        for k in range(2):
            for lt in range(2):
                j = 2 * t + lt
                out[at + 8 * k + j : at + 8 * k + j + 1, :] = (
                    row_sum(acc[k][lt]) * pattern[k, j : j + 1, :]
                )


def first_touched(offsets, k):
    return 2 * ((lax.axis_index(ROW) * 4 + offsets[0, k]) % 64)


def gather_touched(offsets, vector, pattern, ring):
    ring[0:VROWS, :] = vector
    ring[VROWS : VROWS + 8, :] = vector[0:8, :]
    return [ring[pl.ds(first_touched(offsets, k), 8), :] * pattern[k] for k in range(2)]


def assemble(offsets, received, each, at, turn):
    total = None
    for k in range(2):
        for peer in range(PEERS):
            lo = each * peer + at + 8 * k
            part = received[lo : lo + 8, :]
            turn[k, 8 * peer : 8 * peer + 8, :] = part
            turn[k, VROWS + 8 * peer : VROWS + 8 * peer + 8, :] = part
        turned = turn[k, pl.ds(VROWS - 2 * offsets[0, k], VROWS), :]
        total = turned if total is None else total + turned
    return total


def to_all(line, out):
    each = out.shape[0] // PEERS
    value = line[0:each, :]
    for peer in range(PEERS):
        out[each * peer : each * (peer + 1), :] = value


def peer_total(received, each, lo, hi):
    total = received[lo:hi, :]
    for peer in range(1, PEERS):
        total = total + received[each * peer + lo : each * peer + hi, :]
    return total


def lane_total(a):
    return jnp.sum(a, axis=1, keepdims=True)


def full_total(a):
    return lane_total(row_sum(a))


def full_max(a):
    return jnp.max(jnp.max(a, axis=0, keepdims=True), axis=1, keepdims=True)


def packed(values):
    lane = lax.broadcasted_iota(jnp.int32, (1, LANES), 1)
    row = jnp.zeros((1, LANES), f32)
    for n, value in enumerate(values):
        row = jnp.where(lane == n, value, row)
    return row


def products_of(offsets, vector, mats, pattern, ring, line):
    touched = gather_touched(offsets, vector, pattern, ring)
    forward(mats[0], touched, line, 0)
    forward(mats[1], touched, line, 8)


def first_products(
    offsets_in, pattern_in, A_in, G_in, x_in, out, pat_out, A, G,
    offsets, pattern, line, ring, small_sems, sems,
):
    small = [
        pltpu.make_async_copy(offsets_in, offsets, small_sems.at[0]),
        pltpu.make_async_copy(pattern_in, pattern, small_sems.at[1]),
        pltpu.make_async_copy(x_in, ring.at[0:VROWS, :], small_sems.at[2]),
        pltpu.make_async_copy(x_in.at[0:8, :], ring.at[VROWS : VROWS + 8, :], small_sems.at[3]),
    ]
    big = [
        [pltpu.make_async_copy(src.at[t], dst.at[t], sems.at[m, t]) for t in range(4)]
        for m, (src, dst) in enumerate(((G_in, G), (A_in, A)))
    ]
    for copy in small + big[0] + big[1]:
        copy.start()
    for copy in small:
        copy.wait()
    for k in range(2):
        for t in range(4):
            pat_out[k, 2 * t : 2 * t + 2, :] = jnp.full((2, LANES), pattern[k, t].astype(f32))
    touched = [ring[pl.ds(first_touched(offsets, k), 8), :] * pat_out[k] for k in range(2)]
    for m, mat in enumerate((G, A)):
        for t in range(4):
            big[m][t].wait()
            forward_row(mat, t, touched, line, 8 * m)
    to_all(line, out)


def start_rows(z, y, gx, ax):
    return rho_step * z - y - rho_step * ax, -gx


def first_start(A, G, pat, recv, z, y, out, gx_out, ax_out, line):
    gx = peer_total(recv, 16, 0, 8)
    ax = peer_total(recv, 16, 8, 16)
    gx_out[...] = gx
    ax_out[...] = ax
    va, vg = start_rows(z[...], y[...], gx, ax)
    backward(((A, va), (G, vg)), pat, line, 0)
    to_all(line, out)


def begin_solve(offsets, A, G, pat, recv, x, diag, lin, out, rem_out, *rest, dual):
    if dual:
        dual_out, line, ring, turn = rest
    else:
        line, ring, turn = rest
    each = 32 if dual else 16
    start = assemble(offsets, recv, each, 0, turn)
    xv = x[...]
    shifted = diag[...] + sigma_shift
    rem = sigma_shift * xv - lin[...] - shifted * xv + start
    rem_out[...] = rem
    products_of(offsets, rem, (G, A), pat, ring, line)
    line[16:17, :] = packed((full_total(rem * rem), full_total(rem * shifted * rem)))
    to_all(line, out)
    if dual:
        residual = diag[...] * xv + lin[...] + assemble(offsets, recv, each, 16, turn)
        dual_out[...] = jnp.max(jnp.abs(residual), axis=0, keepdims=True)


def first_image(A, G, pat, recv, out, gd_out, ad_out, sc_out, line):
    gd = peer_total(recv, 17, 0, 8)
    ad = peer_total(recv, 17, 8, 16)
    gd_out[...] = gd
    ad_out[...] = ad
    sc_out[...] = peer_total(recv, 17, 16, 17)
    backward(((G, gd), (A, rho_step * ad)), pat, line, 0)
    line[16:17, :] = row_sum(gd * gd + rho_step * (ad * ad))
    to_all(line, out)


def first_step(
    offsets, A, G, pat, recv, direction, sc, diag, out, rem_out, step_out, line, ring, turn
):
    image_part = assemble(offsets, recv, 17, 0, turn)
    squares = lane_total(peer_total(recv, 17, 16, 17))
    norm, weighted = sc[0:1, 0:1], sc[0:1, 1:2]
    step = norm / (squares + weighted)
    d = direction[...]
    shifted = diag[...] + sigma_shift
    rem = d - step * (image_part + shifted * d)
    rem_out[...] = rem
    step_out[...] = jnp.broadcast_to(step, (1, LANES))
    products_of(offsets, rem, (G, A), pat, ring, line)
    weighted_rem = rem * shifted
    line[16:17, :] = packed(
        (full_total(rem * rem), full_total(weighted_rem * rem), full_total(weighted_rem * d))
    )
    to_all(line, out)


def second_images(recv, gd, ad, sc, out, gd_out, ad_out, small_out):
    now = peer_total(recv, 17, 16, 17)
    norm, weighted_rem, weighted_mix = now[:, 0:1], now[:, 1:2], now[:, 2:3]
    norm_old, weighted_old = sc[0:1, 0:1], sc[0:1, 1:2]
    ratio = norm / norm_old
    gd2 = peer_total(recv, 17, 0, 8) + ratio * gd[...]
    ad2 = peer_total(recv, 17, 8, 16) + ratio * ad[...]
    gd_out[...] = gd2
    ad_out[...] = ad2
    weighted = weighted_rem + 2.0 * ratio * weighted_mix + ratio * ratio * weighted_old
    small_out[...] = packed((norm, weighted, ratio))
    squares = row_sum(gd2 * gd2 + rho_step * (ad2 * ad2))
    out[...] = jnp.broadcast_to(squares, (PEERS, LANES))


def update(
    A, G, pat, recv, small, step, gd, ad, gd2, ad2, gx, ax, x, rem, d, z, y, lo, hi,
    *rest, last,
):
    if last:
        diag, lin, primal0, out, x_out, z_out, y_out, base_out, line = rest
    else:
        out, x_out, z_out, y_out, gx_out, ax_out, primal_out, line = rest
    squares = full_total(recv[...])
    norm, weighted, ratio = small[0:1, 0:1], small[0:1, 1:2], small[0:1, 2:3]
    step2 = norm / (squares + weighted)
    step1 = step[0:1, :]
    axv = ax[...]
    tracked = axv + step1 * ad[...] + step2 * ad2[...]
    zv, yv = z[...], y[...]
    blended = relaxation * tracked + (1.0 - relaxation) * zv
    z_new = jnp.minimum(jnp.maximum(blended + yv / rho_step, lo[...]), hi[...])
    y_new = yv + rho_step * (blended - z_new)
    z_out[...] = z_new
    y_out[...] = y_new
    gxv = gx[...]
    gx_new = relaxation * (gxv + step1 * gd[...] + step2 * gd2[...]) + (1.0 - relaxation) * gxv
    ax_new = relaxation * tracked + (1.0 - relaxation) * axv
    primal = full_max(jnp.abs(ax_new - z_new))
    if last:
        backward(((G, gx_new), (A, y_new)), pat, line, 0)
        line[16:17, :] = packed((primal0[0:1, 0:1], primal))
    else:
        gx_out[...] = gx_new
        ax_out[...] = ax_new
        primal_out[...] = jnp.broadcast_to(primal, (1, LANES))
        va, vg = start_rows(z_new, y_new, gx_new, ax_new)
        backward(((A, va), (G, vg)), pat, line, 0)
        backward(((G, gx_new), (A, y_new)), pat, line, 16)
    to_all(line, out)
    dv = d[...]
    xv = x[...]
    solved = xv + step1 * dv + step2 * (rem[...] + ratio * dv)
    x_new = relaxation * solved + (1.0 - relaxation) * xv
    x_out[...] = x_new
    if last:
        base_out[...] = diag[...] * x_new + lin[...]


def last_dual(offsets, recv, base, dual0, out, turn):
    residual = base[...] + assemble(offsets, recv, 17, 0, turn)
    primal = recv[16:17, :]
    for peer in range(1, PEERS):
        primal = jnp.maximum(primal, recv[17 * peer + 16 : 17 * peer + 17, :])
    row = packed(
        (primal[:, 0:1], primal[:, 1:2], full_max(dual0[...]), full_max(jnp.abs(residual)))
    )
    out[...] = jnp.broadcast_to(row, (PEERS, LANES))


def finish(recv, x, z, y, x_out, z_out, y_out, out):
    x_out[...] = x[...]
    z_out[...] = z[...]
    y_out[...] = y[...]
    top = jnp.max(recv[...], axis=0, keepdims=True)
    out[0:1, :] = top[:, 0:2]
    out[1:2, :] = top[:, 2:4]


V = (VROWS, LANES)
R8 = (8, LANES)
ONE = (1, LANES)
RING = (VROWS + 8, LANES)
TURN = (2, 2 * VROWS, LANES)
BLOCKS = (4, 2, BS, BS)


def payload(rows):
    return (PEERS * rows, LANES)


def exchange(a, axes):
    wide = a.reshape(PEERS, 1, -1)
    return lax.all_to_all(wide, axes, 0, 0, tiled=True).reshape(a.shape)


def local(
    constraint_blocks, factor_blocks, band_offsets, block_pattern, cost_linear, cost_diagonal,
    lower, upper, x_start, z_start, y_start,
):
    A, G, offsets = constraint_blocks, factor_blocks, band_offsets
    lin, diag = cost_linear.reshape(V), cost_diagonal.reshape(V)
    lo, hi = lower.reshape(R8), upper.reshape(R8)
    x, z, y = x_start.reshape(V), z_start.reshape(R8), y_start.reshape(R8)

    out, pat, A, G = kernel_call(
        first_products, "first_products", [payload(16), (2, 8, LANES), BLOCKS, BLOCKS],
        [
            pltpu.SMEM((1, 2), jnp.int32), pltpu.SMEM((2, 4), jnp.int32), (16, LANES), RING,
            pltpu.SemaphoreType.DMA((4,)), pltpu.SemaphoreType.DMA((2, 4)),
        ],
        [pl.BlockSpec(memory_space=pltpu.HBM)] * 5,
    )(*[pltpu.with_memory_space_constraint(a, pltpu.HBM) for a in (offsets, block_pattern.T, A, G, x)])
    recv = exchange(out, COL)
    out, gx, ax = kernel_call(first_start, "first_start", [payload(16), R8, R8], [(16, LANES)])(
        A, G, pat, recv, z, y
    )
    primal0 = dual0 = None
    for outer in range(2):
        recv = exchange(out, ROW)
        shapes = [payload(17), V] + ([ONE] if outer else [])

        def body(*refs, dual=bool(outer)):
            begin_solve(*refs, dual=dual)

        got = kernel_call(body, f"begin_solve_{outer}", shapes, [(24, LANES), RING, TURN])(
            offsets, A, G, pat, recv, x, diag, lin
        )
        out, d = got[:2]
        if outer:
            dual0 = got[2]
        recv = exchange(out, COL)
        out, gd, ad, sc = kernel_call(
            first_image, "first_image", [payload(17), R8, R8, ONE], [(24, LANES)]
        )(A, G, pat, recv)
        recv = exchange(out, ROW)
        out, rem, step = kernel_call(
            first_step, "first_step", [payload(17), V, ONE], [(24, LANES), RING, TURN]
        )(offsets, A, G, pat, recv, d, sc, diag)
        recv = exchange(out, COL)
        out, gd2, ad2, small = kernel_call(second_images, "second_images", [payload(1), R8, R8, ONE])(
            recv, gd, ad, sc
        )
        recv = exchange(out, ROW)
        args = (A, G, pat, recv, small, step, gd, ad, gd2, ad2, gx, ax, x, rem, d, z, y, lo, hi)
        if outer == 0:

            def body(*refs):
                update(*refs, last=False)

            out, x, z, y, gx, ax, primal0 = kernel_call(
                body, "update_0", [payload(32), V, R8, R8, R8, R8, ONE], [(32, LANES)]
            )(*args)
        else:

            def body(*refs):
                update(*refs, last=True)

            out, x, z, y, base = kernel_call(
                body, "update_1", [payload(17), V, R8, R8, V], [(24, LANES)]
            )(*args, diag, lin, primal0)
    recv = exchange(out, ROW)
    (out,) = kernel_call(last_dual, "last_dual", [payload(1)], [TURN])(offsets, recv, base, dual0)
    recv = exchange(out, COL)
    x, z, y, residuals = kernel_call(finish, "finish", [V, R8, R8, (2, 2)])(recv, x, z, y)
    return x.reshape(-1), z.reshape(-1), y.reshape(-1), residuals


def solution(mesh):
    torus = Mesh(mesh.devices.reshape(2, 4, 2, 4, 4), ROW + COL)
    in_specs = (
        P(ROW, COL, None, None), P(ROW, COL, None, None), P(COL, None), P(ROW, COL), P(COL), P(COL),
        P(ROW), P(ROW), P(COL), P(ROW), P(ROW),
    )
    out_specs = (P(COL), P(ROW), P(ROW), P())
    return jax.shard_map(local, mesh=torus, in_specs=in_specs, out_specs=out_specs, check_vma=False)
```

```python
import jax
import jax.numpy as jnp
from jax import lax
from jax.experimental import pallas as pl
from jax.experimental.pallas import tpu as pltpu
from jax.sharding import Mesh
from jax.sharding import PartitionSpec as P

BS = 256
LANES = 128
ROW = ("row_0", "row_1", "row_2")
COL = ("col_0", "col_1")
PEERS = 16
VROWS = 128

sigma_shift = 1e-06
rho_step = 0.1
relaxation = 1.6

f32 = jnp.float32
VMEM = pl.BlockSpec(memory_space=pltpu.VMEM)


def kernel_call(body, name, outs, scratch=(), spaces=None):
    def call(*arrays):
        return pl.pallas_call(
            body,
            name=name,
            out_shape=[jax.ShapeDtypeStruct(s, f32) for s in outs],
            in_specs=spaces or [VMEM] * len(arrays),
            out_specs=[VMEM] * len(outs),
            scratch_shapes=[pltpu.VMEM(s, f32) if isinstance(s, tuple) else s for s in scratch],
            compiler_params=pltpu.CompilerParams(vmem_limit_bytes=8 << 20),
        )(*arrays)

    return call


def row_sum(a):
    return jnp.sum(a, axis=0, keepdims=True)


def forward_row(mat, t, touched, out, at):
    for ha in range(2):
        acc = None
        for k in range(2):
            for lt in range(2):
                j = 2 * t + lt
                tile = mat[t, k, ha * LANES : (ha + 1) * LANES, lt * LANES : (lt + 1) * LANES]
                term = tile * touched[k][j : j + 1, :]
                acc = term if acc is None else acc + term
        j = at + 2 * t + ha
        out[j : j + 1, :] = row_sum(acc.T)


def forward(mat, touched, out, at):
    for t in range(4):
        forward_row(mat, t, touched, out, at)


def backward(pairs, pattern, out, at):
    for t in range(4):
        acc = [[None, None], [None, None]]
        for mat, v in pairs:
            for ha in range(2):
                j = 2 * t + ha
                column = jnp.broadcast_to(v[j : j + 1, :], (LANES, LANES)).T
                for k in range(2):
                    for lt in range(2):
                        tile = mat[t, k, ha * LANES : (ha + 1) * LANES, lt * LANES : (lt + 1) * LANES]
                        part = (tile * column).reshape(16, 8, LANES).sum(axis=0)
                        acc[k][lt] = part if acc[k][lt] is None else acc[k][lt] + part
        for k in range(2):
            for lt in range(2):
                j = 2 * t + lt
                out[at + 8 * k + j : at + 8 * k + j + 1, :] = (
                    row_sum(acc[k][lt]) * pattern[k, j : j + 1, :]
                )


def first_touched(offsets, k):
    return 2 * ((lax.axis_index(ROW) * 4 + offsets[0, k]) % 64)


def gather_touched(offsets, vector, pattern, ring):
    ring[0:VROWS, :] = vector
    ring[VROWS : VROWS + 8, :] = vector[0:8, :]
    return [ring[pl.ds(first_touched(offsets, k), 8), :] * pattern[k] for k in range(2)]


def assemble(offsets, received, each, at, turn):
    total = None
    for k in range(2):
        for peer in range(PEERS):
            lo = each * peer + at + 8 * k
            part = received[lo : lo + 8, :]
            turn[k, 8 * peer : 8 * peer + 8, :] = part
            turn[k, VROWS + 8 * peer : VROWS + 8 * peer + 8, :] = part
        turned = turn[k, pl.ds(VROWS - 2 * offsets[0, k], VROWS), :]
        total = turned if total is None else total + turned
    return total


def to_all(line, out):
    each = out.shape[0] // PEERS
    value = line[0:each, :]
    for peer in range(PEERS):
        out[each * peer : each * (peer + 1), :] = value


def peer_total(received, each, lo, hi):
    total = received[lo:hi, :]
    for peer in range(1, PEERS):
        total = total + received[each * peer + lo : each * peer + hi, :]
    return total


def lane_total(a):
    return jnp.sum(a, axis=1, keepdims=True)


def full_total(a):
    return lane_total(row_sum(a))


def full_max(a):
    return jnp.max(jnp.max(a, axis=0, keepdims=True), axis=1, keepdims=True)


def packed(values):
    lane = lax.broadcasted_iota(jnp.int32, (1, LANES), 1)
    row = jnp.zeros((1, LANES), f32)
    for n, value in enumerate(values):
        row = jnp.where(lane == n, value, row)
    return row


def products_of(offsets, vector, mats, pattern, ring, line):
    touched = gather_touched(offsets, vector, pattern, ring)
    forward(mats[0], touched, line, 0)
    forward(mats[1], touched, line, 8)


def first_products(
    offsets_in, pattern_in, A_in, G_in, x_in, out, pat_out, A, G,
    offsets, pattern, line, ring, small_sems, sems,
):
    small = [
        pltpu.make_async_copy(offsets_in, offsets, small_sems.at[0]),
        pltpu.make_async_copy(pattern_in, pattern, small_sems.at[1]),
        pltpu.make_async_copy(x_in, ring.at[0:VROWS, :], small_sems.at[2]),
        pltpu.make_async_copy(x_in.at[0:8, :], ring.at[VROWS : VROWS + 8, :], small_sems.at[3]),
    ]
    big = [
        [pltpu.make_async_copy(src.at[t], dst.at[t], sems.at[m, t]) for t in range(4)]
        for m, (src, dst) in enumerate(((G_in, G), (A_in, A)))
    ]
    for copy in small + big[0] + big[1]:
        copy.start()
    for copy in small:
        copy.wait()
    for k in range(2):
        for t in range(4):
            pat_out[k, 2 * t : 2 * t + 2, :] = jnp.full((2, LANES), pattern[k, t].astype(f32))
    touched = [ring[pl.ds(first_touched(offsets, k), 8), :] * pat_out[k] for k in range(2)]
    for m, mat in enumerate((G, A)):
        for t in range(4):
            big[m][t].wait()
            forward_row(mat, t, touched, line, 8 * m)
    to_all(line, out)


def start_rows(z, y, gx, ax):
    return rho_step * z - y - rho_step * ax, -gx


def first_start(A, G, pat, recv, z, y, out, gx_out, ax_out, line):
    gx = peer_total(recv, 16, 0, 8)
    ax = peer_total(recv, 16, 8, 16)
    gx_out[...] = gx
    ax_out[...] = ax
    va, vg = start_rows(z[...], y[...], gx, ax)
    backward(((A, va), (G, vg)), pat, line, 0)
    to_all(line, out)


def begin_solve(offsets, A, G, pat, recv, x, diag, lin, *rest, dual):
    if dual:
        own, out, rem_out, dual_out, line, ring, turn = rest
    else:
        out, rem_out, line, ring, turn = rest
    each = 24 if dual else 16
    start = assemble(offsets, recv, each, 0, turn)
    xv = x[...]
    shifted = diag[...] + sigma_shift
    rem = sigma_shift * xv - lin[...] - shifted * xv + start
    rem_out[...] = rem
    products_of(offsets, rem, (G, A), pat, ring, line)
    line[16:17, :] = packed((full_total(rem * rem), full_total(rem * shifted * rem)))
    to_all(line, out)
    if dual:
        base = diag[...] * xv + lin[...]
        ring[0:VROWS, :] = base
        ring[VROWS : VROWS + 8, :] = base[0:8, :]
        mine = ring[pl.ds(first_touched(offsets, 0), 8), :]
        dual_out[...] = jnp.abs(mine + own[...] + peer_total(recv, 24, 16, 24))


def to_owners(offsets, line, spread, out):
    shift = (offsets[0, 1] - offsets[0, 0]) % 64
    spread[0:8, :] = jnp.zeros((8, LANES), f32)
    spread[8:16, :] = line[24:32, :]
    spread[16:24, :] = jnp.zeros((8, LANES), f32)
    inner = 2 * (shift % 4)
    near = spread[pl.ds(8 - inner, 8), :]
    far = spread[pl.ds(16 - inner, 8), :]
    owner = (lax.axis_index(ROW) + shift // 4) % PEERS
    for peer in range(PEERS):
        here = jnp.where(owner == peer, 1.0, 0.0)
        after = jnp.where((owner + 1) % PEERS == peer, 1.0, 0.0)
        out[24 * peer + 16 : 24 * peer + 24, :] = here * near + after * far


def first_image(A, G, pat, recv, out, gd_out, ad_out, sc_out, line):
    gd = peer_total(recv, 17, 0, 8)
    ad = peer_total(recv, 17, 8, 16)
    gd_out[...] = gd
    ad_out[...] = ad
    sc_out[...] = peer_total(recv, 17, 16, 17)
    backward(((G, gd), (A, rho_step * ad)), pat, line, 0)
    line[16:17, :] = row_sum(gd * gd + rho_step * (ad * ad))
    to_all(line, out)


def first_step(
    offsets, A, G, pat, recv, direction, sc, diag, out, rem_out, step_out, line, ring, turn
):
    image_part = assemble(offsets, recv, 17, 0, turn)
    squares = lane_total(peer_total(recv, 17, 16, 17))
    norm, weighted = sc[0:1, 0:1], sc[0:1, 1:2]
    step = norm / (squares + weighted)
    d = direction[...]
    shifted = diag[...] + sigma_shift
    rem = d - step * (image_part + shifted * d)
    rem_out[...] = rem
    step_out[...] = jnp.broadcast_to(step, (1, LANES))
    products_of(offsets, rem, (G, A), pat, ring, line)
    weighted_rem = rem * shifted
    line[16:17, :] = packed(
        (full_total(rem * rem), full_total(weighted_rem * rem), full_total(weighted_rem * d))
    )
    to_all(line, out)


def second_images(recv, gd, ad, sc, out, gd_out, ad_out, small_out):
    now = peer_total(recv, 17, 16, 17)
    norm, weighted_rem, weighted_mix = now[:, 0:1], now[:, 1:2], now[:, 2:3]
    norm_old, weighted_old = sc[0:1, 0:1], sc[0:1, 1:2]
    ratio = norm / norm_old
    gd2 = peer_total(recv, 17, 0, 8) + ratio * gd[...]
    ad2 = peer_total(recv, 17, 8, 16) + ratio * ad[...]
    gd_out[...] = gd2
    ad_out[...] = ad2
    weighted = weighted_rem + 2.0 * ratio * weighted_mix + ratio * ratio * weighted_old
    small_out[...] = packed((norm, weighted, ratio))
    squares = row_sum(gd2 * gd2 + rho_step * (ad2 * ad2))
    out[...] = jnp.broadcast_to(squares, (PEERS, LANES))


def update(
    A, G, pat, recv, small, step, gd, ad, gd2, ad2, gx, ax, x, rem, d, z, y, lo, hi, *rest, last,
):
    if last:
        diag, lin, primal0, dual0, out, x_out, z_out, y_out, base_out, line = rest
    else:
        offsets, out, x_out, z_out, y_out, gx_out, ax_out, primal_out, own_out, line, spread = rest
    squares = full_total(recv[...])
    norm, weighted, ratio = small[0:1, 0:1], small[0:1, 1:2], small[0:1, 2:3]
    step2 = norm / (squares + weighted)
    step1 = step[0:1, :]
    axv = ax[...]
    tracked = axv + step1 * ad[...] + step2 * ad2[...]
    zv, yv = z[...], y[...]
    blended = relaxation * tracked + (1.0 - relaxation) * zv
    z_new = jnp.minimum(jnp.maximum(blended + yv / rho_step, lo[...]), hi[...])
    y_new = yv + rho_step * (blended - z_new)
    z_out[...] = z_new
    y_out[...] = y_new
    gxv = gx[...]
    gx_new = relaxation * (gxv + step1 * gd[...] + step2 * gd2[...]) + (1.0 - relaxation) * gxv
    ax_new = relaxation * tracked + (1.0 - relaxation) * axv
    primal = full_max(jnp.abs(ax_new - z_new))
    if last:
        backward(((G, gx_new), (A, y_new)), pat, line, 0)
        line[16:17, :] = packed((primal0[0:1, 0:1], primal, full_max(dual0[...])))
        to_all(line, out)
    else:
        gx_out[...] = gx_new
        ax_out[...] = ax_new
        primal_out[...] = jnp.broadcast_to(primal, (1, LANES))
        va, _ = start_rows(z_new, y_new, gx_new, ax_new)
        backward(((G, gx_new),), pat, line, 32)
        backward(((A, va),), pat, line, 0)
        backward(((A, y_new),), pat, line, 16)
        both = line[32:48, :]
        line[16:32, :] = line[16:32, :] + both
        own_out[...] = line[16:24, :]
        start = line[0:16, :] - both
        for peer in range(PEERS):
            out[24 * peer : 24 * peer + 16, :] = start
        to_owners(offsets, line, spread, out)
    dv = d[...]
    xv = x[...]
    solved = xv + step1 * dv + step2 * (rem[...] + ratio * dv)
    x_new = relaxation * solved + (1.0 - relaxation) * xv
    x_out[...] = x_new
    if last:
        base_out[...] = diag[...] * x_new + lin[...]


def last_dual(offsets, recv, base, out, turn):
    residual = base[...] + assemble(offsets, recv, 17, 0, turn)
    top = recv[16:17, :]
    for peer in range(1, PEERS):
        top = jnp.maximum(top, recv[17 * peer + 16 : 17 * peer + 17, :])
    row = packed((top[:, 0:1], top[:, 1:2], top[:, 2:3], full_max(jnp.abs(residual))))
    out[...] = jnp.broadcast_to(row, (PEERS, LANES))


def finish(recv, x, z, y, x_out, z_out, y_out, out):
    x_out[...] = x[...]
    z_out[...] = z[...]
    y_out[...] = y[...]
    top = jnp.max(recv[...], axis=0, keepdims=True)
    out[0:1, :] = top[:, 0:2]
    out[1:2, :] = top[:, 2:4]


V = (VROWS, LANES)
R8 = (8, LANES)
ONE = (1, LANES)
RING = (VROWS + 8, LANES)
TURN = (2, 2 * VROWS, LANES)
BLOCKS = (4, 2, BS, BS)


def payload(rows):
    return (PEERS * rows, LANES)


def exchange(a, axes):
    wide = a.reshape(PEERS, 1, -1)
    return lax.all_to_all(wide, axes, 0, 0, tiled=True).reshape(a.shape)


def near_rows():
    groups = []
    for col in range(16):
        near, far = list(range(0, 8)), list(range(8, 16))
        groups.append([16 * row + col for row in near] + [16 * row + (col ^ 2) for row in far])
    return groups


def exchange_near(a):
    wide = a.reshape(PEERS, 1, -1)
    got = lax.all_to_all(wide, ROW + COL, 0, 0, axis_index_groups=near_rows(), tiled=True)
    return got.reshape(a.shape)


def local(
    constraint_blocks, factor_blocks, band_offsets, block_pattern, cost_linear, cost_diagonal,
    lower, upper, x_start, z_start, y_start,
):
    A, G, offsets = constraint_blocks, factor_blocks, band_offsets
    lin, diag = cost_linear.reshape(V), cost_diagonal.reshape(V)
    lo, hi = lower.reshape(R8), upper.reshape(R8)
    x, z, y = x_start.reshape(V), z_start.reshape(R8), y_start.reshape(R8)

    out, pat, A, G = kernel_call(
        first_products, "first_products", [payload(16), (2, 8, LANES), BLOCKS, BLOCKS],
        [
            pltpu.SMEM((1, 2), jnp.int32), pltpu.SMEM((2, 4), jnp.int32), (16, LANES), RING,
            pltpu.SemaphoreType.DMA((4,)), pltpu.SemaphoreType.DMA((2, 4)),
        ],
        [pl.BlockSpec(memory_space=pltpu.HBM)] * 5,
    )(*[pltpu.with_memory_space_constraint(a, pltpu.HBM) for a in (offsets, block_pattern.T, A, G, x)])
    recv = exchange(out, COL)
    out, gx, ax = kernel_call(first_start, "first_start", [payload(16), R8, R8], [(16, LANES)])(
        A, G, pat, recv, z, y
    )
    primal0 = dual0 = None
    for outer in range(2):
        recv = exchange(out, ROW)
        shapes = [payload(17), V] + ([R8] if outer else [])

        def body(*refs, dual=bool(outer)):
            begin_solve(*refs, dual=dual)

        got = kernel_call(body, f"begin_solve_{outer}", shapes, [(24, LANES), RING, TURN])(
            offsets, A, G, pat, recv, x, diag, lin, *([own] if outer else [])
        )
        out, d = got[:2]
        if outer:
            dual0 = got[2]
        recv = exchange(out, COL)
        out, gd, ad, sc = kernel_call(
            first_image, "first_image", [payload(17), R8, R8, ONE], [(24, LANES)]
        )(A, G, pat, recv)
        recv = exchange(out, ROW)
        out, rem, step = kernel_call(
            first_step, "first_step", [payload(17), V, ONE], [(24, LANES), RING, TURN]
        )(offsets, A, G, pat, recv, d, sc, diag)
        recv = exchange(out, COL)
        out, gd2, ad2, small = kernel_call(second_images, "second_images", [payload(1), R8, R8, ONE])(
            recv, gd, ad, sc
        )
        recv = exchange_near(out)
        args = (A, G, pat, recv, small, step, gd, ad, gd2, ad2, gx, ax, x, rem, d, z, y, lo, hi)
        if outer == 0:

            def body(*refs):
                update(*refs, last=False)

            out, x, z, y, gx, ax, primal0, own = kernel_call(
                body, "update_0", [payload(24), V, R8, R8, R8, R8, ONE, R8],
                [(48, LANES), (24, LANES)],
            )(*args, offsets)
        else:

            def body(*refs):
                update(*refs, last=True)

            out, x, z, y, base = kernel_call(
                body, "update_1", [payload(17), V, R8, R8, V], [(24, LANES)]
            )(*args, diag, lin, primal0, dual0)
    recv = exchange(out, ROW)
    (out,) = kernel_call(last_dual, "last_dual", [payload(1)], [TURN])(offsets, recv, base)
    recv = exchange(out, COL)
    x, z, y, residuals = kernel_call(finish, "finish", [V, R8, R8, (2, 2)])(recv, x, z, y)
    return x.reshape(-1), z.reshape(-1), y.reshape(-1), residuals


def solution(mesh):
    torus = Mesh(mesh.devices.reshape(2, 4, 2, 4, 4), ROW + COL)
    in_specs = (
        P(ROW, COL, None, None), P(ROW, COL, None, None), P(COL, None), P(ROW, COL), P(COL), P(COL),
        P(ROW), P(ROW), P(COL), P(ROW), P(ROW),
    )
    out_specs = (P(COL), P(ROW), P(ROW), P())
    return jax.shard_map(local, mesh=torus, in_specs=in_specs, out_specs=out_specs, check_vma=False)
```

```python
import jax
import jax.numpy as jnp
from jax import lax
from jax.experimental import pallas as pl
from jax.experimental.pallas import tpu as pltpu
from jax.sharding import Mesh
from jax.sharding import PartitionSpec as P

BS = 256
LANES = 128
ROW = ("row_0", "row_1", "row_2")
COL = ("col_0", "col_1")
PEERS = 16
VROWS = 128

sigma_shift = 1e-06
rho_step = 0.1
relaxation = 1.6

f32 = jnp.float32
VMEM = pl.BlockSpec(memory_space=pltpu.VMEM)


def kernel_call(body, name, outs, scratch=(), spaces=None):
    def call(*arrays):
        return pl.pallas_call(
            body,
            name=name,
            out_shape=[jax.ShapeDtypeStruct(s, f32) for s in outs],
            in_specs=spaces or [VMEM] * len(arrays),
            out_specs=[VMEM] * len(outs),
            scratch_shapes=[pltpu.VMEM(s, f32) if isinstance(s, tuple) else s for s in scratch],
            compiler_params=pltpu.CompilerParams(vmem_limit_bytes=8 << 20),
        )(*arrays)

    return call


def row_sum(a):
    return jnp.sum(a, axis=0, keepdims=True)


def forward_row(mat, t, touched, out, at):
    for ha in range(2):
        acc = None
        for k in range(2):
            for lt in range(2):
                j = 2 * t + lt
                tile = mat[t, k, ha * LANES : (ha + 1) * LANES, lt * LANES : (lt + 1) * LANES]
                term = tile * touched[k][j : j + 1, :]
                acc = term if acc is None else acc + term
        j = at + 2 * t + ha
        out[j : j + 1, :] = row_sum(acc.T)


def forward(mat, touched, out, at):
    for t in range(4):
        forward_row(mat, t, touched, out, at)


def backward(pairs, pattern, out, at):
    for t in range(4):
        acc = [[None, None], [None, None]]
        for mat, v in pairs:
            for ha in range(2):
                j = 2 * t + ha
                column = jnp.broadcast_to(v[j : j + 1, :], (LANES, LANES)).T
                for k in range(2):
                    for lt in range(2):
                        tile = mat[t, k, ha * LANES : (ha + 1) * LANES, lt * LANES : (lt + 1) * LANES]
                        part = (tile * column).reshape(16, 8, LANES).sum(axis=0)
                        acc[k][lt] = part if acc[k][lt] is None else acc[k][lt] + part
        for k in range(2):
            for lt in range(2):
                j = 2 * t + lt
                out[at + 8 * k + j : at + 8 * k + j + 1, :] = (
                    row_sum(acc[k][lt]) * pattern[k, j : j + 1, :]
                )


def first_touched(offsets, k):
    return 2 * ((lax.axis_index(ROW) * 4 + offsets[0, k]) % 64)


def gather_touched(offsets, vector, pattern, ring):
    ring[0:VROWS, :] = vector
    ring[VROWS : VROWS + 8, :] = vector[0:8, :]
    return [ring[pl.ds(first_touched(offsets, k), 8), :] * pattern[k] for k in range(2)]


def assemble(offsets, received, each, at, turn):
    total = None
    for k in range(2):
        for peer in range(PEERS):
            lo = each * peer + at + 8 * k
            part = received[lo : lo + 8, :]
            turn[k, 8 * peer : 8 * peer + 8, :] = part
            turn[k, VROWS + 8 * peer : VROWS + 8 * peer + 8, :] = part
        turned = turn[k, pl.ds(VROWS - 2 * offsets[0, k], VROWS), :]
        total = turned if total is None else total + turned
    return total


def to_all(line, out):
    each = out.shape[0] // PEERS
    value = line[0:each, :]
    for peer in range(PEERS):
        out[each * peer : each * (peer + 1), :] = value


def peer_total(received, each, lo, hi):
    total = received[lo:hi, :]
    for peer in range(1, PEERS):
        total = total + received[each * peer + lo : each * peer + hi, :]
    return total


def lane_total(a):
    return jnp.sum(a, axis=1, keepdims=True)


def full_total(a):
    return lane_total(row_sum(a))


def full_max(a):
    return jnp.max(jnp.max(a, axis=0, keepdims=True), axis=1, keepdims=True)


def packed(values):
    lane = lax.broadcasted_iota(jnp.int32, (1, LANES), 1)
    row = jnp.zeros((1, LANES), f32)
    for n, value in enumerate(values):
        row = jnp.where(lane == n, value, row)
    return row


def products_of(offsets, vector, mats, pattern, ring, line):
    touched = gather_touched(offsets, vector, pattern, ring)
    forward(mats[0], touched, line, 0)
    forward(mats[1], touched, line, 8)


def first_products(
    offsets_in, pattern_in, A_in, G_in, x_in, out, pat_out, A, G,
    offsets, pattern, line, ring, small_sems, sems,
):
    small = [
        pltpu.make_async_copy(offsets_in, offsets, small_sems.at[0]),
        pltpu.make_async_copy(pattern_in, pattern, small_sems.at[1]),
        pltpu.make_async_copy(x_in, ring.at[0:VROWS, :], small_sems.at[2]),
    ]
    big = [
        pltpu.make_async_copy(src, dst, sems.at[m])
        for m, (src, dst) in enumerate(((G_in, G), (A_in, A)))
    ]
    for copy in small + big:
        copy.start()
    for copy in small:
        copy.wait()
    ring[VROWS : VROWS + 8, :] = ring[0:8, :]
    for k in range(2):
        for t in range(4):
            pat_out[k, 2 * t : 2 * t + 2, :] = jnp.full((2, LANES), pattern[k, t].astype(f32))
    touched = [ring[pl.ds(first_touched(offsets, k), 8), :] * pat_out[k] for k in range(2)]
    for m, mat in enumerate((G, A)):
        big[m].wait()
        forward(mat, touched, line, 8 * m)
    to_all(line, out)


def start_rows(z, y, gx, ax):
    return rho_step * z - y - rho_step * ax, -gx


def first_start(A, G, pat, recv, z, y, out, gx_out, ax_out, line):
    gx = peer_total(recv, 16, 0, 8)
    ax = peer_total(recv, 16, 8, 16)
    gx_out[...] = gx
    ax_out[...] = ax
    va, vg = start_rows(z[...], y[...], gx, ax)
    backward(((A, va), (G, vg)), pat, line, 0)
    to_all(line, out)


def begin_solve(offsets, A, G, pat, recv, x, diag, lin, *rest, dual):
    if dual:
        own, out, rem_out, dual_out, line, ring, turn = rest
    else:
        out, rem_out, line, ring, turn = rest
    each = 24 if dual else 16
    start = assemble(offsets, recv, each, 0, turn)
    xv = x[...]
    shifted = diag[...] + sigma_shift
    rem = sigma_shift * xv - lin[...] - shifted * xv + start
    rem_out[...] = rem
    products_of(offsets, rem, (G, A), pat, ring, line)
    line[16:17, :] = packed((full_total(rem * rem), full_total(rem * shifted * rem)))
    to_all(line, out)
    if dual:
        base = diag[...] * xv + lin[...]
        ring[0:VROWS, :] = base
        ring[VROWS : VROWS + 8, :] = base[0:8, :]
        mine = ring[pl.ds(first_touched(offsets, 0), 8), :]
        dual_out[...] = jnp.abs(mine + own[...] + peer_total(recv, 24, 16, 24))


def to_owners(offsets, line, spread, out):
    shift = (offsets[0, 1] - offsets[0, 0]) % 64
    spread[0:8, :] = jnp.zeros((8, LANES), f32)
    spread[8:16, :] = line[24:32, :]
    spread[16:24, :] = jnp.zeros((8, LANES), f32)
    inner = 2 * (shift % 4)
    near = spread[pl.ds(8 - inner, 8), :]
    far = spread[pl.ds(16 - inner, 8), :]
    owner = (lax.axis_index(ROW) + shift // 4) % PEERS
    for peer in range(PEERS):
        here = jnp.where(owner == peer, 1.0, 0.0)
        after = jnp.where((owner + 1) % PEERS == peer, 1.0, 0.0)
        out[24 * peer + 16 : 24 * peer + 24, :] = here * near + after * far


def first_image(A, G, pat, recv, out, gd_out, ad_out, sc_out, line):
    gd = peer_total(recv, 17, 0, 8)
    ad = peer_total(recv, 17, 8, 16)
    gd_out[...] = gd
    ad_out[...] = ad
    sc_out[...] = peer_total(recv, 17, 16, 17)
    backward(((G, gd), (A, rho_step * ad)), pat, line, 0)
    line[16:17, :] = row_sum(gd * gd + rho_step * (ad * ad))
    to_all(line, out)


def first_step(
    offsets, A, G, pat, recv, direction, sc, diag, out, rem_out, step_out, line, ring, turn
):
    image_part = assemble(offsets, recv, 17, 0, turn)
    squares = lane_total(peer_total(recv, 17, 16, 17))
    norm, weighted = sc[0:1, 0:1], sc[0:1, 1:2]
    step = norm / (squares + weighted)
    d = direction[...]
    shifted = diag[...] + sigma_shift
    rem = d - step * (image_part + shifted * d)
    rem_out[...] = rem
    step_out[...] = jnp.broadcast_to(step, (1, LANES))
    products_of(offsets, rem, (G, A), pat, ring, line)
    weighted_rem = rem * shifted
    line[16:17, :] = packed(
        (full_total(rem * rem), full_total(weighted_rem * rem), full_total(weighted_rem * d))
    )
    to_all(line, out)


def second_images(recv, gd, ad, sc, out, gd_out, ad_out, small_out):
    now = peer_total(recv, 17, 16, 17)
    norm, weighted_rem, weighted_mix = now[:, 0:1], now[:, 1:2], now[:, 2:3]
    norm_old, weighted_old = sc[0:1, 0:1], sc[0:1, 1:2]
    ratio = norm / norm_old
    gd2 = peer_total(recv, 17, 0, 8) + ratio * gd[...]
    ad2 = peer_total(recv, 17, 8, 16) + ratio * ad[...]
    gd_out[...] = gd2
    ad_out[...] = ad2
    weighted = weighted_rem + 2.0 * ratio * weighted_mix + ratio * ratio * weighted_old
    small_out[...] = packed((norm, weighted, ratio))
    squares = row_sum(gd2 * gd2 + rho_step * (ad2 * ad2))
    out[...] = jnp.broadcast_to(squares, (PEERS, LANES))


def update(
    A, G, pat, recv, small, step, gd, ad, gd2, ad2, gx, ax, x, rem, d, z, y, lo, hi, *rest, last,
):
    if last:
        diag, lin, primal0, dual0, out, x_out, z_out, y_out, base_out, line = rest
    else:
        offsets, out, x_out, z_out, y_out, gx_out, ax_out, primal_out, own_out, line, spread = rest
    squares = full_total(recv[...])
    norm, weighted, ratio = small[0:1, 0:1], small[0:1, 1:2], small[0:1, 2:3]
    step2 = norm / (squares + weighted)
    step1 = step[0:1, :]
    axv = ax[...]
    tracked = axv + step1 * ad[...] + step2 * ad2[...]
    zv, yv = z[...], y[...]
    blended = relaxation * tracked + (1.0 - relaxation) * zv
    z_new = jnp.minimum(jnp.maximum(blended + yv / rho_step, lo[...]), hi[...])
    y_new = yv + rho_step * (blended - z_new)
    z_out[...] = z_new
    y_out[...] = y_new
    gxv = gx[...]
    gx_new = relaxation * (gxv + step1 * gd[...] + step2 * gd2[...]) + (1.0 - relaxation) * gxv
    ax_new = relaxation * tracked + (1.0 - relaxation) * axv
    primal = full_max(jnp.abs(ax_new - z_new))
    if last:
        backward(((G, gx_new), (A, y_new)), pat, line, 0)
        line[16:17, :] = packed((primal0[0:1, 0:1], primal, full_max(dual0[...])))
        to_all(line, out)
    else:
        gx_out[...] = gx_new
        ax_out[...] = ax_new
        primal_out[...] = jnp.broadcast_to(primal, (1, LANES))
        va, _ = start_rows(z_new, y_new, gx_new, ax_new)
        backward(((G, gx_new),), pat, line, 32)
        backward(((A, va),), pat, line, 0)
        backward(((A, y_new),), pat, line, 16)
        both = line[32:48, :]
        line[16:32, :] = line[16:32, :] + both
        own_out[...] = line[16:24, :]
        start = line[0:16, :] - both
        for peer in range(PEERS):
            out[24 * peer : 24 * peer + 16, :] = start
        to_owners(offsets, line, spread, out)
    dv = d[...]
    xv = x[...]
    solved = xv + step1 * dv + step2 * (rem[...] + ratio * dv)
    x_new = relaxation * solved + (1.0 - relaxation) * xv
    x_out[...] = x_new
    if last:
        base_out[...] = diag[...] * x_new + lin[...]


def last_dual(offsets, recv, base, out, turn):
    residual = base[...] + assemble(offsets, recv, 17, 0, turn)
    top = recv[16:17, :]
    for peer in range(1, PEERS):
        top = jnp.maximum(top, recv[17 * peer + 16 : 17 * peer + 17, :])
    row = packed((top[:, 0:1], top[:, 1:2], top[:, 2:3], full_max(jnp.abs(residual))))
    out[...] = jnp.broadcast_to(row, (PEERS, LANES))


def finish(recv, x, z, y, x_out, z_out, y_out, out):
    x_out[...] = x[...]
    z_out[...] = z[...]
    y_out[...] = y[...]
    top = jnp.max(recv[...], axis=0, keepdims=True)
    out[0:1, :] = top[:, 0:2]
    out[1:2, :] = top[:, 2:4]


V = (VROWS, LANES)
R8 = (8, LANES)
ONE = (1, LANES)
RING = (VROWS + 8, LANES)
TURN = (2, 2 * VROWS, LANES)
BLOCKS = (4, 2, BS, BS)


def payload(rows):
    return (PEERS * rows, LANES)


def exchange(a, axes):
    wide = a.reshape(PEERS, 1, -1)
    return lax.all_to_all(wide, axes, 0, 0, tiled=True).reshape(a.shape)


def near_rows():
    groups = []
    for col in range(16):
        near, far = list(range(0, 8)), list(range(8, 16))
        groups.append([16 * row + col for row in near] + [16 * row + (col ^ 2) for row in far])
    return groups


def exchange_near(a):
    wide = a.reshape(PEERS, 1, -1)
    got = lax.all_to_all(wide, ROW + COL, 0, 0, axis_index_groups=near_rows(), tiled=True)
    return got.reshape(a.shape)


def local(
    constraint_blocks, factor_blocks, band_offsets, block_pattern, cost_linear, cost_diagonal,
    lower, upper, x_start, z_start, y_start,
):
    A, G, offsets = constraint_blocks, factor_blocks, band_offsets
    lin, diag = cost_linear.reshape(V), cost_diagonal.reshape(V)
    lo, hi = lower.reshape(R8), upper.reshape(R8)
    x, z, y = x_start.reshape(V), z_start.reshape(R8), y_start.reshape(R8)

    out, pat, A, G = kernel_call(
        first_products, "first_products", [payload(16), (2, 8, LANES), BLOCKS, BLOCKS],
        [
            pltpu.SMEM((1, 2), jnp.int32), pltpu.SMEM((2, 4), jnp.int32), (16, LANES), RING,
            pltpu.SemaphoreType.DMA((3,)), pltpu.SemaphoreType.DMA((2,)),
        ],
        [pl.BlockSpec(memory_space=pltpu.HBM)] * 5,
    )(*[pltpu.with_memory_space_constraint(a, pltpu.HBM) for a in (offsets, block_pattern.T, A, G, x)])
    recv = exchange(out, COL)
    out, gx, ax = kernel_call(first_start, "first_start", [payload(16), R8, R8], [(16, LANES)])(
        A, G, pat, recv, z, y
    )
    primal0 = dual0 = None
    for outer in range(2):
        recv = exchange(out, ROW)
        shapes = [payload(17), V] + ([R8] if outer else [])

        def body(*refs, dual=bool(outer)):
            begin_solve(*refs, dual=dual)

        got = kernel_call(body, f"begin_solve_{outer}", shapes, [(24, LANES), RING, TURN])(
            offsets, A, G, pat, recv, x, diag, lin, *([own] if outer else [])
        )
        out, d = got[:2]
        if outer:
            dual0 = got[2]
        recv = exchange(out, COL)
        out, gd, ad, sc = kernel_call(
            first_image, "first_image", [payload(17), R8, R8, ONE], [(24, LANES)]
        )(A, G, pat, recv)
        recv = exchange(out, ROW)
        out, rem, step = kernel_call(
            first_step, "first_step", [payload(17), V, ONE], [(24, LANES), RING, TURN]
        )(offsets, A, G, pat, recv, d, sc, diag)
        recv = exchange(out, COL)
        out, gd2, ad2, small = kernel_call(second_images, "second_images", [payload(1), R8, R8, ONE])(
            recv, gd, ad, sc
        )
        recv = exchange_near(out)
        args = (A, G, pat, recv, small, step, gd, ad, gd2, ad2, gx, ax, x, rem, d, z, y, lo, hi)
        if outer == 0:

            def body(*refs):
                update(*refs, last=False)

            out, x, z, y, gx, ax, primal0, own = kernel_call(
                body, "update_0", [payload(24), V, R8, R8, R8, R8, ONE, R8],
                [(48, LANES), (24, LANES)],
            )(*args, offsets)
        else:

            def body(*refs):
                update(*refs, last=True)

            out, x, z, y, base = kernel_call(
                body, "update_1", [payload(17), V, R8, R8, V], [(24, LANES)]
            )(*args, diag, lin, primal0, dual0)
    recv = exchange(out, ROW)
    (out,) = kernel_call(last_dual, "last_dual", [payload(1)], [TURN])(offsets, recv, base)
    recv = exchange(out, COL)
    x, z, y, residuals = kernel_call(finish, "finish", [V, R8, R8, (2, 2)])(recv, x, z, y)
    return x.reshape(-1), z.reshape(-1), y.reshape(-1), residuals


def solution(mesh):
    torus = Mesh(mesh.devices.reshape(2, 4, 2, 4, 4), ROW + COL)
    in_specs = (
        P(ROW, COL, None, None), P(ROW, COL, None, None), P(COL, None), P(ROW, COL), P(COL), P(COL),
        P(ROW), P(ROW), P(COL), P(ROW), P(ROW),
    )
    out_specs = (P(COL), P(ROW), P(ROW), P())
    return jax.shard_map(local, mesh=torus, in_specs=in_specs, out_specs=out_specs, check_vma=False)
```

```python
import jax
import jax.numpy as jnp
from jax import lax
from jax.experimental import pallas as pl
from jax.experimental.pallas import tpu as pltpu
from jax.sharding import Mesh
from jax.sharding import PartitionSpec as P

BS = 256
LANES = 128
ROW = ("row_0", "row_1", "row_2")
COL = ("col_0", "col_1")
PEERS = 16
VROWS = 128

sigma_shift = 1e-06
rho_step = 0.1
relaxation = 1.6

f32 = jnp.float32
VMEM = pl.BlockSpec(memory_space=pltpu.VMEM)


def kernel_call(body, name, outs, scratch=(), spaces=None):
    def call(*arrays):
        return pl.pallas_call(
            body,
            name=name,
            out_shape=[jax.ShapeDtypeStruct(s, f32) for s in outs],
            in_specs=spaces or [VMEM] * len(arrays),
            out_specs=[VMEM] * len(outs),
            scratch_shapes=[pltpu.VMEM(s, f32) if isinstance(s, tuple) else s for s in scratch],
            compiler_params=pltpu.CompilerParams(vmem_limit_bytes=8 << 20),
        )(*arrays)

    return call


def row_sum(a):
    return jnp.sum(a, axis=0, keepdims=True)


def forward_row(mat, t, touched, out, at):
    for ha in range(2):
        acc = None
        for k in range(2):
            for lt in range(2):
                j = 2 * t + lt
                tile = mat[t, k, ha * LANES : (ha + 1) * LANES, lt * LANES : (lt + 1) * LANES]
                term = tile * touched[k][j : j + 1, :]
                acc = term if acc is None else acc + term
        j = at + 2 * t + ha
        out[j : j + 1, :] = row_sum(acc.T)


def forward(mat, touched, out, at):
    for t in range(4):
        forward_row(mat, t, touched, out, at)


def backward(pairs, pattern, out, at):
    for t in range(4):
        acc = [[None, None], [None, None]]
        for mat, v in pairs:
            for ha in range(2):
                j = 2 * t + ha
                column = jnp.broadcast_to(v[j : j + 1, :], (LANES, LANES)).T
                for k in range(2):
                    for lt in range(2):
                        tile = mat[t, k, ha * LANES : (ha + 1) * LANES, lt * LANES : (lt + 1) * LANES]
                        part = (tile * column).reshape(16, 8, LANES).sum(axis=0)
                        acc[k][lt] = part if acc[k][lt] is None else acc[k][lt] + part
        for k in range(2):
            for lt in range(2):
                j = 2 * t + lt
                out[at + 8 * k + j : at + 8 * k + j + 1, :] = (
                    row_sum(acc[k][lt]) * pattern[k, j : j + 1, :]
                )


def first_touched(offsets, k):
    return 2 * ((lax.axis_index(ROW) * 4 + offsets[0, k]) % 64)


def gather_touched(offsets, vector, pattern, ring):
    ring[0:VROWS, :] = vector
    ring[VROWS : VROWS + 8, :] = vector[0:8, :]
    return [ring[pl.ds(first_touched(offsets, k), 8), :] * pattern[k] for k in range(2)]


def assemble(offsets, received, each, at, turn):
    total = None
    for k in range(2):
        for peer in range(PEERS):
            lo = each * peer + at + 8 * k
            part = received[lo : lo + 8, :]
            turn[k, 8 * peer : 8 * peer + 8, :] = part
            turn[k, VROWS + 8 * peer : VROWS + 8 * peer + 8, :] = part
        turned = turn[k, pl.ds(VROWS - 2 * offsets[0, k], VROWS), :]
        total = turned if total is None else total + turned
    return total


def to_all(line, out):
    each = out.shape[0] // PEERS
    value = line[0:each, :]
    for peer in range(PEERS):
        out[each * peer : each * (peer + 1), :] = value


def peer_total(received, each, lo, hi):
    total = received[lo:hi, :]
    for peer in range(1, PEERS):
        total = total + received[each * peer + lo : each * peer + hi, :]
    return total


def lane_total(a):
    return jnp.sum(a, axis=1, keepdims=True)


def full_total(a):
    return lane_total(row_sum(a))


def full_max(a):
    return jnp.max(jnp.max(a, axis=0, keepdims=True), axis=1, keepdims=True)


def packed(values):
    lane = lax.broadcasted_iota(jnp.int32, (1, LANES), 1)
    row = jnp.zeros((1, LANES), f32)
    for n, value in enumerate(values):
        row = jnp.where(lane == n, value, row)
    return row


def products_of(offsets, vector, mats, pattern, ring, line):
    touched = gather_touched(offsets, vector, pattern, ring)
    forward(mats[0], touched, line, 0)
    forward(mats[1], touched, line, 8)


def first_products(
    offsets_in, pattern_in, A_in, G_in, x_in, out, pat_out, A, G,
    offsets, pattern, line, ring, small_sems, sems,
):
    small = [
        pltpu.make_async_copy(offsets_in, offsets, small_sems.at[0]),
        pltpu.make_async_copy(pattern_in, pattern, small_sems.at[1]),
        pltpu.make_async_copy(x_in, ring.at[0:VROWS, :], small_sems.at[2]),
    ]
    big = [
        pltpu.make_async_copy(src, dst, sems.at[m])
        for m, (src, dst) in enumerate(((G_in, G), (A_in, A)))
    ]
    for copy in small + big:
        copy.start()
    for copy in small:
        copy.wait()
    ring[VROWS : VROWS + 8, :] = ring[0:8, :]
    for k in range(2):
        for t in range(4):
            pat_out[k, 2 * t : 2 * t + 2, :] = jnp.full((2, LANES), pattern[k, t].astype(f32))
    touched = [ring[pl.ds(first_touched(offsets, k), 8), :] * pat_out[k] for k in range(2)]
    for m, mat in enumerate((G, A)):
        big[m].wait()
        forward(mat, touched, line, 8 * m)
    to_all(line, out)


def start_rows(z, y, gx, ax):
    return rho_step * z - y - rho_step * ax, -gx


def first_start(A, G, pat, recv, z, y, out, gx_out, ax_out, line):
    gx = peer_total(recv, 16, 0, 8)
    ax = peer_total(recv, 16, 8, 16)
    gx_out[...] = gx
    ax_out[...] = ax
    va, vg = start_rows(z[...], y[...], gx, ax)
    backward(((A, va), (G, vg)), pat, line, 0)
    to_all(line, out)


def begin_solve(offsets, A, G, pat, recv, x, diag, lin, *rest, dual):
    if dual:
        own, out, rem_out, dual_out, line, ring, turn = rest
    else:
        out, rem_out, line, ring, turn = rest
    each = 24 if dual else 16
    start = assemble(offsets, recv, each, 0, turn)
    xv = x[...]
    shifted = diag[...] + sigma_shift
    rem = sigma_shift * xv - lin[...] - shifted * xv + start
    rem_out[...] = rem
    products_of(offsets, rem, (G, A), pat, ring, line)
    line[16:17, :] = packed((full_total(rem * rem), full_total(rem * shifted * rem)))
    to_all(line, out)
    if dual:
        base = diag[...] * xv + lin[...]
        ring[0:VROWS, :] = base
        ring[VROWS : VROWS + 8, :] = base[0:8, :]
        mine = ring[pl.ds(first_touched(offsets, 0), 8), :]
        dual_out[...] = jnp.abs(mine + own[...] + peer_total(recv, 24, 16, 24))


def to_owners(offsets, line, spread, out):
    shift = (offsets[0, 1] - offsets[0, 0]) % 64
    spread[0:8, :] = jnp.zeros((8, LANES), f32)
    spread[8:16, :] = line[24:32, :]
    spread[16:24, :] = jnp.zeros((8, LANES), f32)
    inner = 2 * (shift % 4)
    near = spread[pl.ds(8 - inner, 8), :]
    far = spread[pl.ds(16 - inner, 8), :]
    owner = (lax.axis_index(ROW) + shift // 4) % PEERS
    for peer in range(PEERS):
        here = jnp.where(owner == peer, 1.0, 0.0)
        after = jnp.where((owner + 1) % PEERS == peer, 1.0, 0.0)
        out[24 * peer + 16 : 24 * peer + 24, :] = here * near + after * far


def first_image(A, G, pat, recv, out, gd_out, ad_out, sc_out, line):
    gd = peer_total(recv, 17, 0, 8)
    ad = peer_total(recv, 17, 8, 16)
    gd_out[...] = gd
    ad_out[...] = ad
    sc_out[...] = peer_total(recv, 17, 16, 17)
    backward(((G, gd), (A, rho_step * ad)), pat, line, 0)
    line[16:17, :] = row_sum(gd * gd + rho_step * (ad * ad))
    to_all(line, out)


def first_step(
    offsets, A, G, pat, recv, direction, sc, diag, out, rem_out, step_out, line, ring, turn
):
    image_part = assemble(offsets, recv, 17, 0, turn)
    squares = lane_total(peer_total(recv, 17, 16, 17))
    norm, weighted = sc[0:1, 0:1], sc[0:1, 1:2]
    step = norm / (squares + weighted)
    d = direction[...]
    shifted = diag[...] + sigma_shift
    rem = d - step * (image_part + shifted * d)
    rem_out[...] = rem
    step_out[...] = jnp.broadcast_to(step, (1, LANES))
    products_of(offsets, rem, (G, A), pat, ring, line)
    weighted_rem = rem * shifted
    line[16:17, :] = packed(
        (full_total(rem * rem), full_total(weighted_rem * rem), full_total(weighted_rem * d))
    )
    to_all(line, out)


def second_images(recv, gd, ad, sc, out, gd_out, ad_out, small_out):
    now = peer_total(recv, 17, 16, 17)
    norm, weighted_rem, weighted_mix = now[:, 0:1], now[:, 1:2], now[:, 2:3]
    norm_old, weighted_old = sc[0:1, 0:1], sc[0:1, 1:2]
    ratio = norm / norm_old
    gd2 = peer_total(recv, 17, 0, 8) + ratio * gd[...]
    ad2 = peer_total(recv, 17, 8, 16) + ratio * ad[...]
    gd_out[...] = gd2
    ad_out[...] = ad2
    weighted = weighted_rem + 2.0 * ratio * weighted_mix + ratio * ratio * weighted_old
    small_out[...] = packed((norm, weighted, ratio))
    squares = row_sum(gd2 * gd2 + rho_step * (ad2 * ad2))
    out[...] = jnp.broadcast_to(squares, (PEERS, LANES))


def update(
    A, G, pat, recv, small, step, gd, ad, gd2, ad2, gx, ax, x, rem, d, z, y, lo, hi, *rest, last,
):
    if last:
        diag, lin, primal0, dual0, out, x_out, z_out, y_out, base_out, line = rest
    else:
        offsets, out, x_out, z_out, y_out, gx_out, ax_out, primal_out, own_out, line, spread = rest
    squares = full_total(recv[...])
    norm, weighted, ratio = small[0:1, 0:1], small[0:1, 1:2], small[0:1, 2:3]
    step2 = norm / (squares + weighted)
    step1 = step[0:1, :]
    axv = ax[...]
    tracked = axv + step1 * ad[...] + step2 * ad2[...]
    zv, yv = z[...], y[...]
    blended = relaxation * tracked + (1.0 - relaxation) * zv
    z_new = jnp.minimum(jnp.maximum(blended + yv / rho_step, lo[...]), hi[...])
    y_new = yv + rho_step * (blended - z_new)
    z_out[...] = z_new
    y_out[...] = y_new
    gxv = gx[...]
    gx_new = relaxation * (gxv + step1 * gd[...] + step2 * gd2[...]) + (1.0 - relaxation) * gxv
    ax_new = relaxation * tracked + (1.0 - relaxation) * axv
    primal = full_max(jnp.abs(ax_new - z_new))
    if last:
        backward(((G, gx_new), (A, y_new)), pat, line, 0)
        line[16:17, :] = packed((primal0[0:1, 0:1], primal, full_max(dual0[...])))
        to_all(line, out)
    else:
        gx_out[...] = gx_new
        ax_out[...] = ax_new
        primal_out[...] = jnp.broadcast_to(primal, (1, LANES))
        va, _ = start_rows(z_new, y_new, gx_new, ax_new)
        backward(((G, gx_new),), pat, line, 32)
        backward(((A, va),), pat, line, 0)
        backward(((A, y_new),), pat, line, 16)
        both = line[32:48, :]
        line[16:32, :] = line[16:32, :] + both
        own_out[...] = line[16:24, :]
        start = line[0:16, :] - both
        for peer in range(PEERS):
            out[24 * peer : 24 * peer + 16, :] = start
        to_owners(offsets, line, spread, out)
    dv = d[...]
    xv = x[...]
    solved = xv + step1 * dv + step2 * (rem[...] + ratio * dv)
    x_new = relaxation * solved + (1.0 - relaxation) * xv
    x_out[...] = x_new
    if last:
        base_out[...] = diag[...] * x_new + lin[...]


def last_dual(offsets, recv, base, out, turn):
    residual = base[...] + assemble(offsets, recv, 17, 0, turn)
    top = recv[16:17, :]
    for peer in range(1, PEERS):
        top = jnp.maximum(top, recv[17 * peer + 16 : 17 * peer + 17, :])
    row = packed((top[:, 0:1], top[:, 1:2], top[:, 2:3], full_max(jnp.abs(residual))))
    out[...] = jnp.broadcast_to(row, (PEERS, LANES))


def finish(recv, x, z, y, x_out, z_out, y_out, out):
    x_out[...] = x[...]
    z_out[...] = z[...]
    y_out[...] = y[...]
    top = jnp.max(recv[...], axis=0, keepdims=True)
    out[0:1, :] = top[:, 0:2]
    out[1:2, :] = top[:, 2:4]


V = (VROWS, LANES)
R8 = (8, LANES)
ONE = (1, LANES)
RING = (VROWS + 8, LANES)
TURN = (2, 2 * VROWS, LANES)
BLOCKS = (4, 2, BS, BS)


def payload(rows):
    return (PEERS * rows, LANES)


def exchange(a, axes):
    wide = a.reshape(PEERS, 1, -1)
    return lax.all_to_all(wide, axes, 0, 0, tiled=True).reshape(a.shape)


def near_rows():
    groups = []
    for col in range(16):
        near, far = list(range(0, 8)), list(range(8, 16))
        groups.append([16 * row + col for row in near] + [16 * row + (col ^ 2) for row in far])
    return groups


def exchange_near(a):
    wide = a.reshape(PEERS, 1, -1)
    got = lax.all_to_all(wide, ROW + COL, 0, 0, axis_index_groups=near_rows(), tiled=True)
    return got.reshape(a.shape)


def local(
    constraint_blocks, factor_blocks, band_offsets, block_pattern, cost_linear, cost_diagonal,
    lower, upper, x_start, z_start, y_start,
):
    A, G, offsets = constraint_blocks, factor_blocks, band_offsets
    lin, diag = cost_linear.reshape(V), cost_diagonal.reshape(V)
    lo, hi = lower.reshape(R8), upper.reshape(R8)
    x, z, y = x_start.reshape(V), z_start.reshape(R8), y_start.reshape(R8)

    out, pat, A, G = kernel_call(
        first_products, "first_products", [payload(16), (2, 8, LANES), BLOCKS, BLOCKS],
        [
            pltpu.SMEM((1, 2), jnp.int32), pltpu.SMEM((2, 4), jnp.int32), (16, LANES), RING,
            pltpu.SemaphoreType.DMA((3,)), pltpu.SemaphoreType.DMA((2,)),
        ],
        [pl.BlockSpec(memory_space=pltpu.HBM)] * 5,
    )(*[pltpu.with_memory_space_constraint(a, pltpu.HBM) for a in (offsets, block_pattern.T, A, G, x)])
    recv = exchange(out, COL)
    out, gx, ax = kernel_call(first_start, "first_start", [payload(16), R8, R8], [(16, LANES)])(
        A, G, pat, recv, z, y
    )
    primal0 = dual0 = None
    for outer in range(2):
        recv = exchange(out, ROW)
        shapes = [payload(17), V] + ([R8] if outer else [])

        def body(*refs, dual=bool(outer)):
            begin_solve(*refs, dual=dual)

        got = kernel_call(body, f"begin_solve_{outer}", shapes, [(24, LANES), RING, TURN])(
            offsets, A, G, pat, recv, x, diag, lin, *([own] if outer else [])
        )
        out, d = got[:2]
        if outer:
            dual0 = got[2]
        recv = exchange(out, COL)
        out, gd, ad, sc = kernel_call(
            first_image, "first_image", [payload(17), R8, R8, ONE], [(24, LANES)]
        )(A, G, pat, recv)
        recv = exchange(out, ROW)
        out, rem, step = kernel_call(
            first_step, "first_step", [payload(17), V, ONE], [(24, LANES), RING, TURN]
        )(offsets, A, G, pat, recv, d, sc, diag)
        recv = exchange(out, COL)
        out, gd2, ad2, small = kernel_call(second_images, "second_images", [payload(1), R8, R8, ONE])(
            recv, gd, ad, sc
        )
        recv = exchange(out, ROW) if outer else exchange_near(out)
        args = (A, G, pat, recv, small, step, gd, ad, gd2, ad2, gx, ax, x, rem, d, z, y, lo, hi)
        if outer == 0:

            def body(*refs):
                update(*refs, last=False)

            out, x, z, y, gx, ax, primal0, own = kernel_call(
                body, "update_0", [payload(24), V, R8, R8, R8, R8, ONE, R8],
                [(48, LANES), (24, LANES)],
            )(*args, offsets)
        else:

            def body(*refs):
                update(*refs, last=True)

            out, x, z, y, base = kernel_call(
                body, "update_1", [payload(17), V, R8, R8, V], [(24, LANES)]
            )(*args, diag, lin, primal0, dual0)
    recv = exchange(out, ROW)
    (out,) = kernel_call(last_dual, "last_dual", [payload(1)], [TURN])(offsets, recv, base)
    recv = exchange(out, COL)
    x, z, y, residuals = kernel_call(finish, "finish", [V, R8, R8, (2, 2)])(recv, x, z, y)
    return x.reshape(-1), z.reshape(-1), y.reshape(-1), residuals


def solution(mesh):
    torus = Mesh(mesh.devices.reshape(2, 4, 2, 4, 4), ROW + COL)
    in_specs = (
        P(ROW, COL, None, None), P(ROW, COL, None, None), P(COL, None), P(ROW, COL), P(COL), P(COL),
        P(ROW), P(ROW), P(COL), P(ROW), P(ROW),
    )
    out_specs = (P(COL), P(ROW), P(ROW), P())
    return jax.shard_map(local, mesh=torus, in_specs=in_specs, out_specs=out_specs, check_vma=False)
```
